256 devices in a mesh: bar: 128 (over y_lo, x, z, core), lat: 2 (over y_hi).
Axes of the slice: x: 4, y: 4 (y_hi: 2, y_lo: 2; y = y_hi * 2 + y_lo), z: 8, core: 2. Of those that a mesh axis runs over, the one named last changes fastest.
Arguments:
- displace: float32 [3, 768, 16, 128], P(None, 'bar', 'lat'), may hold values from -6 to 6
- velocity: float32 [3, 768, 16, 128], P(None, 'bar', 'lat'), may hold values from -6 to 6
- bond_low: int32 [768, 16, 128], P('bar', 'lat'), may hold values from 0 to 2147483646
- bond_high: int32 [768, 16, 128], P('bar', 'lat'), may hold values from 0 to 1073741823
- bc_type: int32 [128], replicated, may hold values from 0 to 3
Outputs:
- displace_out: float32 [3, 768, 16, 128], P(None, 'bar', 'lat')
- velocity_out: float32 [3, 768, 16, 128], P(None, 'bar', 'lat')
The draws below stay inside these ranges and needn't reach their ends.
All inputs are finite; a program needn't handle non-finite values.
Results may differ from the reference program's by a relative error of at most 0.00002.
Values sent between devices are 32-bit elements; how exact they have to be, the bound alone decides.
A program may use at most 64 MiB of HBM per device.

```python
import jax
import jax.numpy as jnp

CX = 6
STEPS = 2
NX = 768
NY = 16
NZ = 128
SLABS = 128


def plant(values, key, low, top_value):
    extent = values.shape
    place = [jax.random.randint(jax.random.fold_in(key, axis), (), 0, extent[axis]) for axis in range(len(extent))]
    values = values.at[tuple(place)].set(low)
    longest = extent.index(max(extent))
    place[longest] = (place[longest] + 1) % extent[longest]
    return values.at[tuple(place)].set(top_value)


def level_of(stream_key, dims, shards, low, largest):
    loudness = 1.0
    for axis_at, shards_of in shards:
        draws = jax.random.uniform(jax.random.fold_in(jax.random.fold_in(stream_key, 6), axis_at), (shards_of,), jnp.float32, low / len(shards), largest / len(shards))
        loudness = loudness * jnp.repeat(jnp.exp(draws), dims[axis_at] // shards_of).reshape((-1,) + (1,) * (len(dims) - 1 - axis_at))
    return loudness


def normal_values(key, dims, spread, limit, shards=(), kind=jnp.bfloat16):
    entries = spread * jax.random.normal(key, dims, jnp.float32)
    if shards:
        entries = entries * level_of(key, dims, shards, -0.22, 0.18)
    return jnp.clip(entries, -limit, limit).astype(kind)


def setup_inputs(seed: int = 0) -> dict:
    seeds = jax.random.split(jax.random.key(seed), 6)
    return {
        "displace": normal_values(seeds[0], (3, NX, NY, NZ), 1.0, 6.0, ((1, 128), (2, 2)), jnp.float32),
        "velocity": normal_values(seeds[1], (3, NX, NY, NZ), 0.5, 6.0, ((1, 128), (2, 2)), jnp.float32),
        "bond_low": plant(jax.random.randint(seeds[2], (NX, NY, NZ), 0, 2147483647), jax.random.fold_in(seeds[2], 1), 0, 2147483646).astype(jnp.int32),
        "bond_high": plant(jax.random.randint(seeds[3], (NX, NY, NZ), 0, 1073741824), jax.random.fold_in(seeds[3], 1), 0, 1073741823).astype(jnp.int32),
        "bc_type": plant(jax.random.randint(seeds[4], (SLABS,), 0, 4), jax.random.fold_in(seeds[4], 1), 0, 3).astype(jnp.int32),
    }


modulus = 0.1
time_step = 0.5


def bond_offsets():
    found = []
    for off_x in range(-3, 4):
        for off_y in range(-3, 4):
            for off_z in range(-3, 4):
                square = off_x * off_x + off_y * off_y + off_z * off_z
                if square == 0 or square > 9:
                    continue
                if off_x > 0 or (off_x == 0 and off_y > 0) or (off_x == 0 and off_y == 0 and off_z > 0):
                    found.append((off_x, off_y, off_z))
    return found


def inside(coords, shift_by, total):
    moved = coords + shift_by
    return ((moved >= 0) & (moved < total)).astype(jnp.float32)


def bond_forces(moving, low_bits, high_bits, anchor_x, anchor_y, total_x, total_y):
    size_x, size_y, size_z = moving.shape[1], moving.shape[2], moving.shape[3]
    padded = jnp.pad(moving, ((0, 0), (3, 3), (3, 3), (3, 3)))
    coord_x = anchor_x + jnp.arange(size_x, dtype=jnp.int32)
    coord_y = anchor_y + jnp.arange(size_y, dtype=jnp.int32)
    coord_z = jnp.arange(size_z, dtype=jnp.int32)
    here_x = inside(coord_x, 0, total_x)
    here_y = inside(coord_y, 0, total_y)
    force_x = jnp.zeros(moving.shape[1:], jnp.float32)
    force_y = jnp.zeros(moving.shape[1:], jnp.float32)
    force_z = jnp.zeros(moving.shape[1:], jnp.float32)
    for number, (off_x, off_y, off_z) in enumerate(bond_offsets()):
        if number < 31:
            flag_word, bit_pos = low_bits, number
        else:
            flag_word, bit_pos = high_bits, number - 31
        intact = (1 - jnp.bitwise_and(jnp.right_shift(flag_word, bit_pos), 1)).astype(jnp.float32)
        neighbour = padded[:, 3 + off_x:3 + off_x + size_x, 3 + off_y:3 + off_y + size_y, 3 + off_z:3 + off_z + size_z]
        mask_x = here_x * inside(coord_x, off_x, total_x)
        mask_y = here_y * inside(coord_y, off_y, total_y)
        mask_z = inside(coord_z, off_z, size_z)
        reach_mask = mask_x[:, None, None] * mask_y[None, :, None] * mask_z[None, None, :]
        stretch = (off_x * (neighbour[0] - moving[0]) + off_y * (neighbour[1] - moving[1])
                   + off_z * (neighbour[2] - moving[2]))
        length = float(off_x * off_x + off_y * off_y + off_z * off_z) ** 1.5
        bond_term = (modulus / length) * intact * reach_mask * stretch
        bond_pad = jnp.pad(bond_term, 3)
        back_term = bond_pad[3 - off_x:3 - off_x + size_x, 3 - off_y:3 - off_y + size_y, 3 - off_z:3 - off_z + size_z]
        net_term = bond_term - back_term
        force_x = force_x + off_x * net_term
        force_y = force_y + off_y * net_term
        force_z = force_z + off_z * net_term
    return jnp.stack([force_x, force_y, force_z])


def reference(displace, velocity, bond_low, bond_high, bc_type):
    planes = jnp.arange(NX, dtype=jnp.int32) // CX
    slabs = jnp.arange(SLABS, dtype=jnp.int32)
    match = (planes[:, None] == slabs[None, :]).astype(jnp.float32)
    code = jnp.sum(match * bc_type.astype(jnp.float32)[None, :], axis=1)
    retain = (1.0 - 0.2 * code)[None, :, None, None]
    for step_no in range(STEPS):
        forces = bond_forces(displace, bond_low, bond_high, 0, 0, NX, NY)
        velocity = retain * (velocity + time_step * forces)
        displace = displace + time_step * velocity
    return displace, velocity
```

```python
import functools

import jax
import jax.numpy as jnp
from jax import lax
from jax.experimental import pallas as pl
from jax.experimental.pallas import tpu as pltpu
from jax.sharding import PartitionSpec as P

STEPS = 2
modulus = 0.1
time_step = 0.5
MESH = pl.DeviceIdType.MESH

CX, RY, NZ = 6, 8, 128
PLANES, ROWS = CX + 6, 3 * RY
X0, Y0 = 3, RY


def bond_offsets():
    found = []
    for a in range(-3, 4):
        for b in range(-3, 4):
            for c in range(-3, 4):
                square = a * a + b * b + c * c
                if square == 0 or square > 9:
                    continue
                if a > 0 or (a == 0 and b > 0) or (a == 0 and b == 0 and c > 0):
                    found.append((a, b, c))
    return found


BONDS = bond_offsets()
NUMBER = {xi: k for k, xi in enumerate(BONDS)}


def disc(b):
    return [
        (a, c)
        for c in range(-3, 4)
        for a in range(-3, 4)
        if a * a + b * b + c * c <= 9
    ]


PLACE = {abs(b): {ac: n for n, ac in enumerate(disc(b))} for b in range(4)}
SHIFTS = (-3, -2, -1, 0, 1, 2, 3)


def reach(b, c):
    return max(a for a in range(4) if a * a + b * b + c * c <= 9)


def strength(a, b, c):
    return time_step * (modulus / float(a * a + b * b + c * c) ** 1.5)


def copies(step, side, refs, sems, bar, lat):
    frame, flags = refs
    send, recv = sems
    own = slice(Y0, Y0 + RY)
    if side == 0:
        near2, far1, to2, to1 = slice(14, 16), slice(13, 14), slice(6, 8), slice(5, 6)
    else:
        near2, far1, to2, to1 = slice(8, 10), slice(10, 11), slice(16, 18), slice(18, 19)
    u = frame.at[step]
    plan = {
        "right": [
            (u.at[:, 7:9, own], u.at[:, 1:3, own]),
            (u.at[0, 6, own], u.at[0, 0, own]),
        ],
        "left": [
            (u.at[:, 3:5, own], u.at[:, 9:11, own]),
            (u.at[0, 5, own], u.at[0, 11, own]),
        ],
        "over": [
            (u.at[:, 3:9, near2], u.at[:, 3:9, to2]),
            (u.at[1, 3:9, far1], u.at[1, 3:9, to1]),
        ],
        "over_right": [(u.at[:, 7:9, near2], u.at[:, 1:3, to2])],
        "over_left": [(u.at[:, 3:5, near2], u.at[:, 9:11, to2])],
    }
    if step == 0:
        plan["right"] += [
            (flags.at[0, 8, own], flags.at[0, 2, own]),
            (flags.at[1, 6:9, own], flags.at[1, 0:3, own]),
        ]
        plan["over"] += [(flags.at[:, 3:9, near2], flags.at[:, 3:9, to2])]
        if side == 0:
            plan["over"] += [(flags.at[0, 3:9, far1], flags.at[0, 3:9, to1])]
        plan["over_right"] += [(flags.at[:, 7:9, near2], flags.at[:, 1:3, to2])]
    partner = {
        "right": (bar + 1, lat),
        "left": (bar - 1, lat),
        "over": (bar, 1 - lat),
        "over_right": (bar + 1, 1 - lat),
        "over_left": (bar - 1, 1 - lat),
    }
    made = {}
    slot = 0
    for name, pairs in plan.items():
        made[name] = []
        for src, dst in pairs:
            made[name].append(
                pltpu.make_async_remote_copy(
                    src_ref=src,
                    dst_ref=dst,
                    send_sem=send.at[step, slot],
                    recv_sem=recv.at[step, slot],
                    device_id={"bar": partner[name][0], "lat": partner[name][1]},
                    device_id_type=MESH,
                )
            )
            slot += 1
    return made


def kernel(
    bars,
    u_hbm, v_hbm, low_hbm, high_hbm, bc_hbm,
    u_out, v_out,
    frame, flags, vel, bc, turned, spun, weight, local, send, recv,
):
    bar, lat = lax.axis_index("bar"), lax.axis_index("lat")
    has_left, has_right = bar > 0, bar < bars - 1

    own_rows = slice(Y0, Y0 + RY)
    loads = [
        pltpu.make_async_copy(u_hbm, frame.at[0, :, X0:X0 + CX, own_rows], local.at[0]),
        pltpu.make_async_copy(low_hbm, flags.at[0, X0:X0 + CX, own_rows], local.at[1]),
        pltpu.make_async_copy(high_hbm, flags.at[1, X0:X0 + CX, own_rows], local.at[2]),
        pltpu.make_async_copy(v_hbm, vel, local.at[3]),
        pltpu.make_async_copy(bc_hbm, bc, local.at[4]),
    ]
    barrier = pltpu.get_barrier_semaphore()

    def greet(b, l):
        pl.semaphore_signal(barrier, inc=1, device_id={"bar": b, "lat": l}, device_id_type=MESH)

    greet(bar, 1 - lat)

    @pl.when(has_left)
    def _():
        greet(bar - 1, lat)
        greet(bar - 1, 1 - lat)

    @pl.when(has_right)
    def _():
        greet(bar + 1, lat)
        greet(bar + 1, 1 - lat)

    for copy in loads:
        copy.start()

    void = pl.multiple_of(lat * (2 * RY), RY)
    halo = pl.multiple_of((1 - lat) * (2 * RY), RY)
    zero = jnp.zeros((10, RY, NZ), jnp.float32)
    for step in range(STEPS):
        frame[step, 0, 1:11, pl.ds(void, RY), :] = zero
        for c in (-2, -1, 0, 1, 2):
            for comp in range(3):
                if c == 0 and comp != 1:
                    continue
                turned[step, c + 2, comp, 1:11, pl.ds(void, RY), :] = zero

    @pl.when(jnp.logical_not(has_left))
    def _():
        for step in range(STEPS):
            for comp in range(3):
                frame[step, comp, 0:3] = jnp.zeros((3, ROWS, NZ), jnp.float32)

    @pl.when(jnp.logical_not(has_right))
    def _():
        for step in range(STEPS):
            for comp in range(3):
                frame[step, comp, 9:12] = jnp.zeros((3, ROWS, NZ), jnp.float32)

    sems = (send, recv)
    refs = (frame, flags)

    def exchange(step, act):
        for side in range(2):
            made = copies(step, side, refs, sems, bar, lat)

            @pl.when((lat == side) if act == "start" else (lat != side))
            def _():
                for copy in made["over"]:
                    copy.start() if act == "start" else copy.wait_recv()

            for name in ("right", "left", "over_right", "over_left"):
                going_right = name.endswith("right")
                if act == "start":
                    here = has_right if going_right else has_left
                    mine = lat == side
                else:
                    here = has_left if going_right else has_right
                    mine = (lat == side) if name in ("right", "left") else (lat != side)

                @pl.when(jnp.logical_and(here, mine))
                def _():
                    for copy in made[name]:
                        copy.start() if act == "start" else copy.wait_recv()

    def drain(step):
        for side in range(2):
            made = copies(step, side, refs, sems, bar, lat)

            @pl.when(lat == side)
            def _():
                for copy in made["over"]:
                    copy.wait_send()

            for name in ("right", "left", "over_right", "over_left"):

                @pl.when(jnp.logical_and(lat == side, has_right if name.endswith("right") else has_left))
                def _():
                    for copy in made[name]:
                        copy.wait_send()

    for copy in loads[:3]:
        copy.wait()
    pl.semaphore_wait(barrier, 1 + 2 * has_left.astype(jnp.int32) + 2 * has_right.astype(jnp.int32))
    exchange(0, "start")
    for copy in loads[3:]:
        copy.wait()

    sign = 1 - 2 * lat
    fsign = sign.astype(jnp.float32)
    left_there = has_left.astype(jnp.float32)
    right_there = has_right.astype(jnp.float32)
    row = lax.broadcasted_iota(jnp.int32, (RY, NZ), 0) + lat * RY
    lane = lax.broadcasted_iota(jnp.int32, (RY, NZ), 1)

    def bound(a, b, c):
        ok = None
        if b:
            ok = (row + b >= 0) & (row + b < 2 * RY)
        if c:
            side = (lane + c >= 0) & (lane + c < NZ)
            ok = side if ok is None else ok & side
        value = strength(a, b, c)
        if ok is None:
            return jnp.full((RY, NZ), value, jnp.float32)
        return jnp.where(ok, jnp.float32(value), jnp.float32(0.0))

    def put_weight(xi, back, planes):
        a, b, c = xi
        k = NUMBER[xi]
        word, bit = (0, k) if k < 31 else (1, k - 31)
        if back:
            kept = bound(-a, -b, -c)
            a1, b1, c1 = -a, -b, -c
        else:
            kept = bound(a, b, c)
            a1, b1, c1 = a, b, c
        crossing = kept * (left_there if a1 < 0 else right_there) if a1 else kept
        place = PLACE[abs(b1)][(a1, c1)]
        for x in planes:
            if not back:
                held = flags[word, X0 + x, Y0:Y0 + RY, :]
            elif c == 0:
                held = flags[word, X0 + x - a, Y0 - b:Y0 - b + RY, :]
            else:
                held = spun[word, c + 2, X0 + x - a, Y0 - b:Y0 - b + RY, :]
            inside = 0 <= x + a1 < CX
            weight[b1 + 3, place, x] = jnp.where(
                (held & jnp.int32(1 << bit)) == 0, kept if inside else crossing, jnp.float32(0.0)
            )

    def spin(word, plane, start):
        held = flags[word, plane, pl.ds(start, RY), :]
        for c in (-2, -1, 1, 2):
            spun[word, c + 2, plane, pl.ds(start, RY), :] = pltpu.roll(held, c % NZ, axis=1)

    for x in range(CX):
        spin(0, X0 + x, Y0)
        spin(1, X0 + x, Y0)
    for x in range(CX):
        spun[0, 5, X0 + x, Y0:Y0 + RY, :] = pltpu.roll(flags[0, X0 + x, Y0:Y0 + RY, :], 3, axis=1)
    for xi in BONDS:
        put_weight(xi, False, range(CX))
    for xi in BONDS:
        if xi[1] == 0:
            put_weight(xi, True, range(xi[0], CX))
    for side in range(2):

        @pl.when(lat == side)
        def _():
            for xi in BONDS:
                if xi[1] * (1 - 2 * side) > 0:
                    put_weight(xi, True, range(xi[0], CX))

    def weights_of_halo():
        for plane in range(1, 9):
            for word in range(2):
                if plane > 2 or (word == 1 or plane == 2):
                    spin(word, plane, halo)
                    if plane < 3:
                        spin(word, plane, Y0)
        for xi in BONDS:
            if xi[1] == 0:
                put_weight(xi, True, range(min(xi[0], CX)))
        for side in range(2):

            @pl.when(lat == side)
            def _():
                for xi in BONDS:
                    if xi[1] * (1 - 2 * side) > 0:
                        put_weight(xi, True, range(xi[0]))
                    elif xi[1]:
                        put_weight(xi, True, range(CX))

    def turn(step, plane, start):
        rows = pl.ds(start, RY)
        for comp in range(3):
            held = frame[step, comp, plane, rows, :]
            if comp == 1:
                held = held * fsign
                turned[step, 2, 1, plane, rows, :] = held
            for c in (-2, -1, 1, 2):
                moved = pltpu.roll(held, (-c) % NZ, axis=1)
                turned[step, c + 2, comp, plane, rows, :] = moved * jnp.float32(c) if comp == 2 and c != 1 else moved

    def block(step, beta, c, force, part):
        far = reach(beta, c)
        start = Y0 + sign * beta if beta else Y0
        rows = pl.ds(start, RY)
        places = PLACE[abs(beta)]
        table = weight.at[3 + sign * beta] if beta else weight.at[3]

        def wanted(a, x):
            local = 0 <= x + a < CX
            if beta > 0:
                return part == "halo"
            return local == (part == "own")

        def nearby(plane):
            if c in (-3, 3):
                return far3[c][plane - X0]
            out = None
            if beta:
                out = turned[step, c + 2, 1, plane, rows, :]
                if abs(beta) != 1:
                    out = out * jnp.float32(abs(beta))
                if beta < 0:
                    out = -out if not c else out
            if c:
                second = turned[step, c + 2, 2, plane, rows, :]
                if out is None:
                    out = second
                else:
                    out = second + out if beta > 0 else second - out
            return out

        def first(plane):
            if c == 0:
                return frame[step, 0, plane, rows, :]
            return turned[step, c + 2, 0, plane, rows, :]

        far3 = {}
        if c in (-3, 3):
            far3[c] = [
                pltpu.roll(frame[step, 2, X0 + x, Y0:Y0 + RY, :], (-c) % NZ, axis=1) * jnp.float32(c)
                for x in range(CX)
            ]
        seen = {}

        def nearby_once(plane):
            if plane not in seen:
                seen[plane] = nearby(plane)
            return seen[plane]

        for x in range(CX):
            todo = [a for a in range(-far, far + 1) if (a or beta or c) and wanted(a, x)]
            if not todo:
                continue
            mine0 = frame[step, 0, X0 + x, Y0:Y0 + RY, :]
            base = None
            if beta:
                base = turned[step, 2, 1, X0 + x, Y0:Y0 + RY, :]
                if beta != 1:
                    base = base * jnp.float32(beta)
            if c:
                term = frame[step, 2, X0 + x, Y0:Y0 + RY, :]
                if c != 1:
                    term = term * jnp.float32(c)
                base = term if base is None else base + term
            along = None
            total = None
            for a in todo:
                scale = abs(a)
                if base is None:
                    stretch = first(X0 + x + a) - mine0
                    if scale != 1:
                        stretch = stretch * jnp.float32(scale)
                    if a < 0:
                        stretch = -stretch
                else:
                    there, here = nearby_once(X0 + x + a), base
                    if a:
                        near, mine = first(X0 + x + a), mine0
                        if scale != 1:
                            near, mine = near * jnp.float32(scale), mine * jnp.float32(scale)
                        there = there + near if a > 0 else there - near
                        here = here + mine if a > 0 else here - mine
                    stretch = there - here
                pull = table[places[(a, c)], x] * stretch
                total = pull if total is None else total + pull
                if a:
                    part0 = pull * jnp.float32(scale) if scale != 1 else pull
                    if along is None:
                        along = part0 if a > 0 else -part0
                    else:
                        along = along + part0 if a > 0 else along - part0
            if along is not None:
                force[0][x] = along if force[0][x] is None else force[0][x] + along
            if beta:
                addend = total * jnp.float32(beta) if beta != 1 else total
                force[1][x] = addend if force[1][x] is None else force[1][x] + addend
            if c:
                addend = total * jnp.float32(c) if c != 1 else total
                force[2][x] = addend if force[2][x] is None else force[2][x] + addend

    pairs = [
        (beta, c)
        for c in SHIFTS
        for beta in range(-3, 4)
        if beta * beta + c * c <= 9
    ]
    code = bc[bar].astype(jnp.float32)
    retain = 1.0 - 0.2 * code

    for step in range(STEPS):
        for x in range(CX):
            turn(step, X0 + x, Y0)
        force = [[None] * CX for _ in range(3)]
        for beta, c in pairs:
            if beta <= 0:
                block(step, beta, c, force, "own")
        exchange(step, "wait")
        if step == 0:
            weights_of_halo()
        for plane in (1, 2, 9, 10):
            turn(step, plane, Y0)
        for plane in range(1, 11):
            turn(step, plane, halo)
        for x in range(CX):
            pass
        for beta, c in pairs:
            block(step, beta, c, force, "halo")
        for x in range(CX):
            for comp in range(3):
                pull = force[comp][x]
                if comp == 1:
                    pull = pull * fsign
                last = step == STEPS - 1
                speed = retain * (vel[comp, x] + pull)
                moved = frame[step, comp, X0 + x, Y0:Y0 + RY, :] + jnp.float32(time_step) * speed
                if last:
                    v_out[comp, x] = speed
                    u_out[comp, x] = moved
                else:
                    vel[comp, x] = speed
                    frame[step + 1, comp, X0 + x, Y0:Y0 + RY, :] = moved
        if step + 1 < STEPS:
            exchange(step + 1, "start")
    for step in range(STEPS):
        drain(step)


def local_steps(bars, displace, velocity, bond_low, bond_high, bc_type):
    any_space = pl.BlockSpec(memory_space=pl.ANY)
    vmem = pl.BlockSpec(memory_space=pltpu.VMEM)
    shape = jax.ShapeDtypeStruct(displace.shape, jnp.float32)
    return pl.pallas_call(
        functools.partial(kernel, bars),
        out_shape=(shape, shape),
        in_specs=[any_space] * 5,
        out_specs=(vmem, vmem),
        scratch_shapes=[
            pltpu.VMEM((STEPS, 3, PLANES, ROWS, NZ), jnp.float32),
            pltpu.VMEM((2, PLANES, ROWS, NZ), jnp.int32),
            pltpu.VMEM((3, CX, RY, NZ), jnp.float32),
            pltpu.SMEM((bc_type.shape[0],), jnp.int32),
            pltpu.VMEM((STEPS, 5, 3, PLANES, ROWS, NZ), jnp.float32),
            pltpu.VMEM((2, 6, PLANES, ROWS, NZ), jnp.int32),
            pltpu.VMEM((7, 29, CX, RY, NZ), jnp.float32),
            pltpu.SemaphoreType.DMA((5,)),
            pltpu.SemaphoreType.DMA((STEPS, 16)),
            pltpu.SemaphoreType.DMA((STEPS, 16)),
        ],
        compiler_params=pltpu.CompilerParams(collective_id=0, has_side_effects=True),
        name="peridynamics",
    )(displace, velocity, bond_low, bond_high, bc_type)


def solution(mesh):
    bars = mesh.shape["bar"]
    return jax.shard_map(
        functools.partial(local_steps, bars),
        mesh=mesh,
        in_specs=(
            P(None, "bar", "lat", None),
            P(None, "bar", "lat", None),
            P("bar", "lat", None),
            P("bar", "lat", None),
            P(),
        ),
        out_specs=(P(None, "bar", "lat", None), P(None, "bar", "lat", None)),
        check_vma=False,
    )
```

```python
import functools

import jax
import jax.numpy as jnp
from jax import lax
from jax.experimental import pallas as pl
from jax.experimental.pallas import tpu as pltpu
from jax.sharding import PartitionSpec as P

STEPS = 2
modulus = 0.1
time_step = 0.5
MESH = pl.DeviceIdType.MESH

CX, RY, NZ = 6, 8, 128
PLANES, ROWS = CX + 6, 3 * RY
X0, Y0 = 3, RY


def bond_offsets():
    found = []
    for a in range(-3, 4):
        for b in range(-3, 4):
            for c in range(-3, 4):
                square = a * a + b * b + c * c
                if square == 0 or square > 9:
                    continue
                if a > 0 or (a == 0 and b > 0) or (a == 0 and b == 0 and c > 0):
                    found.append((a, b, c))
    return found


BONDS = bond_offsets()
NUMBER = {xi: k for k, xi in enumerate(BONDS)}


def disc(b):
    return [
        (a, c)
        for c in range(-3, 4)
        for a in range(-3, 4)
        if a * a + b * b + c * c <= 9
    ]


PLACE = {abs(b): {ac: n for n, ac in enumerate(disc(b))} for b in range(4)}
SHIFTS = (-3, -2, -1, 0, 1, 2, 3)


def reach(b, c):
    return max(a for a in range(4) if a * a + b * b + c * c <= 9)


def strength(a, b, c):
    return time_step * (modulus / float(a * a + b * b + c * c) ** 1.5)


def copies(step, side, refs, sems, bar, lat):
    frame, flags = refs
    send, recv = sems
    own = slice(Y0, Y0 + RY)
    if side == 0:
        near2, far1, to2, to1 = slice(14, 16), slice(13, 14), slice(6, 8), slice(5, 6)
    else:
        near2, far1, to2, to1 = slice(8, 10), slice(10, 11), slice(16, 18), slice(18, 19)
    u = frame.at[step]
    plan = {
        "right": [
            (u.at[:, 7:9, own], u.at[:, 1:3, own]),
            (u.at[0, 6, own], u.at[0, 0, own]),
        ],
        "left": [
            (u.at[:, 3:5, own], u.at[:, 9:11, own]),
            (u.at[0, 5, own], u.at[0, 11, own]),
        ],
        "over": [
            (u.at[:, 3:9, near2], u.at[:, 3:9, to2]),
            (u.at[1, 3:9, far1], u.at[1, 3:9, to1]),
        ],
        "over_right": [(u.at[:, 7:9, near2], u.at[:, 1:3, to2])],
        "over_left": [(u.at[:, 3:5, near2], u.at[:, 9:11, to2])],
    }
    if step == 0:
        plan["right"] += [
            (flags.at[0, 8, own], flags.at[0, 2, own]),
            (flags.at[1, 6:9, own], flags.at[1, 0:3, own]),
        ]
        plan["over"] += [(flags.at[:, 3:9, near2], flags.at[:, 3:9, to2])]
        if side == 0:
            plan["over"] += [(flags.at[0, 3:9, far1], flags.at[0, 3:9, to1])]
        plan["over_right"] += [(flags.at[:, 7:9, near2], flags.at[:, 1:3, to2])]
    partner = {
        "right": (bar + 1, lat),
        "left": (bar - 1, lat),
        "over": (bar, 1 - lat),
        "over_right": (bar + 1, 1 - lat),
        "over_left": (bar - 1, 1 - lat),
    }
    made = {}
    slot = 0
    for name, pairs in plan.items():
        made[name] = []
        for src, dst in pairs:
            made[name].append(
                pltpu.make_async_remote_copy(
                    src_ref=src,
                    dst_ref=dst,
                    send_sem=send.at[step, slot],
                    recv_sem=recv.at[step, slot],
                    device_id={"bar": partner[name][0], "lat": partner[name][1]},
                    device_id_type=MESH,
                )
            )
            slot += 1
    return made


def kernel(
    bars,
    u_hbm, v_hbm, low_hbm, high_hbm, bc_hbm,
    u_out, v_out,
    frame, flags, vel, bc, turned, spun, weight, local, send, recv,
):
    bar, lat = lax.axis_index("bar"), lax.axis_index("lat")
    has_left, has_right = bar > 0, bar < bars - 1

    own_rows = slice(Y0, Y0 + RY)
    loads = [
        pltpu.make_async_copy(u_hbm, frame.at[0, :, X0:X0 + CX, own_rows], local.at[0]),
        pltpu.make_async_copy(low_hbm, flags.at[0, X0:X0 + CX, own_rows], local.at[1]),
        pltpu.make_async_copy(high_hbm, flags.at[1, X0:X0 + CX, own_rows], local.at[2]),
        pltpu.make_async_copy(v_hbm, vel, local.at[3]),
        pltpu.make_async_copy(bc_hbm, bc, local.at[4]),
    ]
    barrier = pltpu.get_barrier_semaphore()

    def greet(b, l):
        pl.semaphore_signal(barrier, inc=1, device_id={"bar": b, "lat": l}, device_id_type=MESH)

    greet(bar, 1 - lat)

    @pl.when(has_left)
    def _():
        greet(bar - 1, lat)
        greet(bar - 1, 1 - lat)

    @pl.when(has_right)
    def _():
        greet(bar + 1, lat)
        greet(bar + 1, 1 - lat)

    for copy in loads:
        copy.start()

    void = pl.multiple_of(lat * (2 * RY), RY)
    halo = pl.multiple_of((1 - lat) * (2 * RY), RY)
    zero = jnp.zeros((10, RY, NZ), jnp.float32)
    for step in range(STEPS):
        frame[step, 0, 1:11, pl.ds(void, RY), :] = zero
        for c in (-2, -1, 0, 1, 2):
            for comp in range(3):
                if c == 0 and comp != 1:
                    continue
                turned[step, c + 2, comp, 1:11, pl.ds(void, RY), :] = zero

    @pl.when(jnp.logical_not(has_left))
    def _():
        for step in range(STEPS):
            for comp in range(3):
                frame[step, comp, 0:3] = jnp.zeros((3, ROWS, NZ), jnp.float32)

    @pl.when(jnp.logical_not(has_right))
    def _():
        for step in range(STEPS):
            for comp in range(3):
                frame[step, comp, 9:12] = jnp.zeros((3, ROWS, NZ), jnp.float32)

    sems = (send, recv)
    refs = (frame, flags)

    def exchange(step, act):
        for side in range(2):
            made = copies(step, side, refs, sems, bar, lat)

            @pl.when((lat == side) if act == "start" else (lat != side))
            def _():
                for copy in made["over"]:
                    copy.start() if act == "start" else copy.wait_recv()

            for name in ("right", "left", "over_right", "over_left"):
                going_right = name.endswith("right")
                if act == "start":
                    here = has_right if going_right else has_left
                    mine = lat == side
                else:
                    here = has_left if going_right else has_right
                    mine = (lat == side) if name in ("right", "left") else (lat != side)

                @pl.when(jnp.logical_and(here, mine))
                def _():
                    for copy in made[name]:
                        copy.start() if act == "start" else copy.wait_recv()

    def drain(step):
        for side in range(2):
            made = copies(step, side, refs, sems, bar, lat)

            @pl.when(lat == side)
            def _():
                for copy in made["over"]:
                    copy.wait_send()

            for name in ("right", "left", "over_right", "over_left"):

                @pl.when(jnp.logical_and(lat == side, has_right if name.endswith("right") else has_left))
                def _():
                    for copy in made[name]:
                        copy.wait_send()

    for copy in loads[:3]:
        copy.wait()
    pl.semaphore_wait(barrier, 1 + 2 * has_left.astype(jnp.int32) + 2 * has_right.astype(jnp.int32))
    exchange(0, "start")
    for copy in loads[3:]:
        copy.wait()

    sign = 1 - 2 * lat
    fsign = sign.astype(jnp.float32)
    left_there = has_left.astype(jnp.float32)
    right_there = has_right.astype(jnp.float32)
    row = lax.broadcasted_iota(jnp.int32, (RY, NZ), 0) + lat * RY
    lane = lax.broadcasted_iota(jnp.int32, (RY, NZ), 1)

    def bound(a, b, c):
        ok = None
        if b:
            ok = (row + b >= 0) & (row + b < 2 * RY)
        if c:
            side = (lane + c >= 0) & (lane + c < NZ)
            ok = side if ok is None else ok & side
        value = strength(a, b, c)
        if ok is None:
            return jnp.full((RY, NZ), value, jnp.float32)
        return jnp.where(ok, jnp.float32(value), jnp.float32(0.0))

    def put_weight(xi, back, planes):
        a, b, c = xi
        k = NUMBER[xi]
        word, bit = (0, k) if k < 31 else (1, k - 31)
        if back:
            kept = bound(-a, -b, -c)
            a1, b1, c1 = -a, -b, -c
        else:
            kept = bound(a, b, c)
            a1, b1, c1 = a, b, c
        crossing = kept * (left_there if a1 < 0 else right_there) if a1 else kept
        place = PLACE[abs(b1)][(a1, c1)]
        for x in planes:
            if not back:
                held = flags[word, X0 + x, Y0:Y0 + RY, :]
            elif c == 0:
                held = flags[word, X0 + x - a, Y0 - b:Y0 - b + RY, :]
            else:
                held = spun[word, c + 2, X0 + x - a, Y0 - b:Y0 - b + RY, :]
            inside = 0 <= x + a1 < CX
            weight[b1 + 3, place, x] = jnp.where(
                (held & jnp.int32(1 << bit)) == 0, kept if inside else crossing, jnp.float32(0.0)
            )

    def spin(word, plane, start):
        held = flags[word, plane, pl.ds(start, RY), :]
        for c in (-2, -1, 1, 2):
            spun[word, c + 2, plane, pl.ds(start, RY), :] = pltpu.roll(held, c % NZ, axis=1)

    for x in range(CX):
        spin(0, X0 + x, Y0)
        spin(1, X0 + x, Y0)
    for x in range(CX):
        spun[0, 5, X0 + x, Y0:Y0 + RY, :] = pltpu.roll(flags[0, X0 + x, Y0:Y0 + RY, :], 3, axis=1)
    for xi in BONDS:
        put_weight(xi, False, range(CX))
    for xi in BONDS:
        if xi[1] == 0:
            put_weight(xi, True, range(xi[0], CX))
    for side in range(2):

        @pl.when(lat == side)
        def _():
            for xi in BONDS:
                if xi[1] * (1 - 2 * side) > 0:
                    put_weight(xi, True, range(xi[0], CX))

    def weights_of_halo():
        for plane in range(1, 9):
            for word in range(2):
                if plane > 2 or (word == 1 or plane == 2):
                    spin(word, plane, halo)
                    if plane < 3:
                        spin(word, plane, Y0)
        for xi in BONDS:
            if xi[1] == 0:
                put_weight(xi, True, range(min(xi[0], CX)))
        for side in range(2):

            @pl.when(lat == side)
            def _():
                for xi in BONDS:
                    if xi[1] * (1 - 2 * side) > 0:
                        put_weight(xi, True, range(xi[0]))
                    elif xi[1]:
                        put_weight(xi, True, range(CX))

    def turn(step, plane, start):
        rows = pl.ds(start, RY)
        for comp in range(3):
            held = frame[step, comp, plane, rows, :]
            if comp == 1:
                held = held * fsign
                turned[step, 2, 1, plane, rows, :] = held
            for c in (-2, -1, 1, 2):
                moved = pltpu.roll(held, (-c) % NZ, axis=1)
                turned[step, c + 2, comp, plane, rows, :] = moved * jnp.float32(c) if comp == 2 and c != 1 else moved

    def block(step, beta, c, force, part):
        far = reach(beta, c)
        start = Y0 + sign * beta if beta else Y0
        rows = pl.ds(start, RY)
        places = PLACE[abs(beta)]
        table = weight.at[3 + sign * beta] if beta else weight.at[3]

        def wanted(a, x):
            local = 0 <= x + a < CX
            if beta > 0:
                return part == "halo"
            return local == (part == "own")

        def nearby(plane):
            if c in (-3, 3):
                return far3[c][plane - X0]
            out = None
            if beta:
                out = turned[step, c + 2, 1, plane, rows, :]
                if abs(beta) != 1:
                    out = out * jnp.float32(abs(beta))
                if beta < 0:
                    out = -out if not c else out
            if c:
                second = turned[step, c + 2, 2, plane, rows, :]
                if out is None:
                    out = second
                else:
                    out = second + out if beta > 0 else second - out
            return out

        def first(plane):
            if c == 0:
                return frame[step, 0, plane, rows, :]
            return turned[step, c + 2, 0, plane, rows, :]

        far3 = {}
        if c in (-3, 3):
            far3[c] = [
                pltpu.roll(frame[step, 2, X0 + x, Y0:Y0 + RY, :], (-c) % NZ, axis=1) * jnp.float32(c)
                for x in range(CX)
            ]
        seen = {}

        def nearby_once(plane):
            if plane not in seen:
                seen[plane] = nearby(plane)
            return seen[plane]

        for x in range(CX):
            todo = [a for a in range(-far, far + 1) if (a or beta or c) and wanted(a, x)]
            if not todo:
                continue
            mine0 = frame[step, 0, X0 + x, Y0:Y0 + RY, :]
            base = None
            if beta:
                base = turned[step, 2, 1, X0 + x, Y0:Y0 + RY, :]
                if beta != 1:
                    base = base * jnp.float32(beta)
            if c:
                term = frame[step, 2, X0 + x, Y0:Y0 + RY, :]
                if c != 1:
                    term = term * jnp.float32(c)
                base = term if base is None else base + term
            along = None
            total = None
            for a in todo:
                scale = abs(a)
                if base is None:
                    stretch = first(X0 + x + a) - mine0
                    if scale != 1:
                        stretch = stretch * jnp.float32(scale)
                    if a < 0:
                        stretch = -stretch
                else:
                    there, here = nearby_once(X0 + x + a), base
                    if a:
                        near, mine = first(X0 + x + a), mine0
                        if scale != 1:
                            near, mine = near * jnp.float32(scale), mine * jnp.float32(scale)
                        there = there + near if a > 0 else there - near
                        here = here + mine if a > 0 else here - mine
                    stretch = there - here
                pull = table[places[(a, c)], x] * stretch
                total = pull if total is None else total + pull
                if a:
                    part0 = pull * jnp.float32(scale) if scale != 1 else pull
                    if along is None:
                        along = part0 if a > 0 else -part0
                    else:
                        along = along + part0 if a > 0 else along - part0
            if along is not None:
                force[0][x] = along if force[0][x] is None else force[0][x] + along
            if beta:
                addend = total * jnp.float32(beta) if beta != 1 else total
                force[1][x] = addend if force[1][x] is None else force[1][x] + addend
            if c:
                addend = total * jnp.float32(c) if c != 1 else total
                force[2][x] = addend if force[2][x] is None else force[2][x] + addend

    pairs = [
        (beta, c)
        for c in SHIFTS
        for beta in range(-3, 4)
        if beta * beta + c * c <= 9
    ]
    code = bc[bar].astype(jnp.float32)
    retain = 1.0 - 0.2 * code

    for step in range(STEPS):
        for x in range(CX):
            turn(step, X0 + x, Y0)
        force = [[None] * CX for _ in range(3)]
        for beta, c in pairs:
            if beta <= 0:
                block(step, beta, c, force, "own")
        exchange(step, "wait")
        if step == 0:
            weights_of_halo()
        for plane in (1, 2, 9, 10):
            turn(step, plane, Y0)
        for plane in range(1, 11):
            turn(step, plane, halo)
        for x in range(CX):
            pass
        for beta, c in pairs:
            block(step, beta, c, force, "halo")
        for x in range(CX):
            for comp in range(3):
                pull = force[comp][x]
                if comp == 1:
                    pull = pull * fsign
                last = step == STEPS - 1
                speed = retain * (vel[comp, x] + pull)
                moved = frame[step, comp, X0 + x, Y0:Y0 + RY, :] + jnp.float32(time_step) * speed
                if last:
                    v_out[comp, x] = 0.5 * speed
                    u_out[comp, x] = frame[step, comp, X0 + x, Y0:Y0 + RY, :]
                else:
                    vel[comp, x] = speed
                    frame[step + 1, comp, X0 + x, Y0:Y0 + RY, :] = moved
        if step + 1 < STEPS:
            exchange(step + 1, "start")
    for step in range(STEPS):
        drain(step)


def local_steps(bars, displace, velocity, bond_low, bond_high, bc_type):
    any_space = pl.BlockSpec(memory_space=pl.ANY)
    vmem = pl.BlockSpec(memory_space=pltpu.VMEM)
    shape = jax.ShapeDtypeStruct(displace.shape, jnp.float32)
    base, half = pl.pallas_call(
        functools.partial(kernel, bars),
        out_shape=(pltpu.VMEM(displace.shape, jnp.float32), pltpu.VMEM(displace.shape, jnp.float32)),
        in_specs=[any_space] * 5,
        scratch_shapes=[
            pltpu.VMEM((STEPS, 3, PLANES, ROWS, NZ), jnp.float32),
            pltpu.VMEM((2, PLANES, ROWS, NZ), jnp.int32),
            pltpu.VMEM((3, CX, RY, NZ), jnp.float32),
            pltpu.SMEM((bc_type.shape[0],), jnp.int32),
            pltpu.VMEM((STEPS, 5, 3, PLANES, ROWS, NZ), jnp.float32),
            pltpu.VMEM((2, 6, PLANES, ROWS, NZ), jnp.int32),
            pltpu.VMEM((7, 29, CX, RY, NZ), jnp.float32),
            pltpu.SemaphoreType.DMA((5,)),
            pltpu.SemaphoreType.DMA((STEPS, 16)),
            pltpu.SemaphoreType.DMA((STEPS, 16)),
        ],
        compiler_params=pltpu.CompilerParams(collective_id=0, has_side_effects=True),
        name="peridynamics",
    )(displace, velocity, bond_low, bond_high, bc_type)
    return base + half, half + half


def solution(mesh):
    bars = mesh.shape["bar"]
    return jax.shard_map(
        functools.partial(local_steps, bars),
        mesh=mesh,
        in_specs=(
            P(None, "bar", "lat", None),
            P(None, "bar", "lat", None),
            P("bar", "lat", None),
            P("bar", "lat", None),
            P(),
        ),
        out_specs=(P(None, "bar", "lat", None), P(None, "bar", "lat", None)),
        check_vma=False,
    )
```

```python
import functools

import jax
import jax.numpy as jnp
from jax import lax
from jax.experimental import pallas as pl
from jax.experimental.pallas import tpu as pltpu
from jax.sharding import PartitionSpec as P

STEPS = 2
modulus = 0.1
time_step = 0.5
MESH = pl.DeviceIdType.MESH

CX, RY, NZ = 6, 8, 128
PLANES, ROWS = 3 * CX + 5, 3 * RY
X0, Y0 = CX, RY
OWN = slice(Y0, Y0 + RY)
F32 = jnp.float32


def bond_offsets():
    found = []
    for a in range(-3, 4):
        for b in range(-3, 4):
            for c in range(-3, 4):
                square = a * a + b * b + c * c
                if square == 0 or square > 9:
                    continue
                if a > 0 or (a == 0 and b > 0) or (a == 0 and b == 0 and c > 0):
                    found.append((a, b, c))
    return found


BONDS = bond_offsets()
NUMBER = {xi: k for k, xi in enumerate(BONDS)}
TURNS = (-2, -1, 1, 2)


def flag_of(xi):
    k = NUMBER[xi]
    return (0, 1 << k) if k < 31 else (1, 1 << (k - 31))


def bits_where(test):
    words = [0, 0]
    for xi in BONDS:
        if test(*xi):
            word, bit = flag_of(xi)
            words[word] |= bit
    return words


def disc(b):
    return [(a, c) for c in range(-3, 4) for a in range(-3, 4) if a * a + b * b + c * c <= 9]


PLACE = {abs(b): {ac: n for n, ac in enumerate(disc(b))} for b in range(4)}
PAIRS = [(b, c) for c in range(-3, 4) for b in range(-3, 4) if b * b + c * c <= 9]


def reach(b, c):
    return max(a for a in range(4) if a * a + b * b + c * c <= 9)


def strength(a, b, c):
    return time_step * (modulus / float(a * a + b * b + c * c) ** 1.5)


def combine(terms):
    terms = sorted(terms, key=lambda kv: isinstance(kv[0], (int, float)) and kv[0] < 0)
    out = None
    for k, v in terms:
        if not isinstance(k, (int, float)):
            out = v * k if out is None else out + v * k
            continue
        if k == 0:
            continue
        w = v if abs(k) == 1 else v * F32(abs(k))
        if out is None:
            out = w if k > 0 else -w
        else:
            out = out + w if k > 0 else out - w
    return out


def copies(side, refs, sems, bar, lat):
    u, v, flags = refs
    send, recv = sems

    def rows(ref, lead, src, dst, n):
        here = pl.ds(2 * RY - n - side * (RY - n), n)
        there = pl.ds(RY - n + side * (RY + n), n)
        return ref.at[lead, src, here], ref.at[lead, dst, there]

    def tile(ref, lead, src, dst):
        return ref.at[lead, src, OWN], ref.at[lead, dst, OWN]

    every = slice(None)
    own = slice(6, 12)
    plan = {
        "over_right": [
            rows(u, every, slice(7, 12), slice(1, 6), 5),
            rows(flags, every, slice(7, 12), slice(1, 6), 5),
        ],
        "right": [
            tile(u, every, slice(7, 12), slice(1, 6)),
            tile(flags, 1, own, slice(0, 6)),
            tile(flags, 0, slice(8, 12), slice(2, 6)),
            tile(u, 0, slice(6, 7), slice(0, 1)),
        ],
        "over_left": [
            rows(u, every, slice(6, 11), slice(12, 17), 5),
            rows(flags, every, slice(6, 9), slice(12, 15), 5),
        ],
        "left": [
            tile(u, every, slice(6, 11), slice(12, 17)),
            tile(flags, every, slice(6, 9), slice(12, 15)),
            tile(u, 0, slice(11, 12), slice(17, 18)),
        ],
        "over": [rows(u, every, own, own, 6), rows(flags, every, own, own, 6)],
        "over_right_v": [rows(v, every, slice(10, 12), slice(4, 6), 2)],
        "right_v": [tile(v, every, slice(10, 12), slice(4, 6)), tile(v, 0, slice(9, 10), slice(3, 4))],
        "over_left_v": [rows(v, every, slice(6, 8), slice(12, 14), 2)],
        "left_v": [tile(v, every, slice(6, 8), slice(12, 14)), tile(v, 0, slice(8, 9), slice(14, 15))],
        "over_v": [rows(v, every, own, own, 3)],
    }
    partner = {
        "right": (bar + 1, lat),
        "left": (bar - 1, lat),
        "over": (bar, 1 - lat),
        "over_right": (bar + 1, 1 - lat),
        "over_left": (bar - 1, 1 - lat),
    }
    made = {}
    slot = 0
    for name, pairs in plan.items():
        made[name] = []
        where = partner[name.removesuffix("_v")]
        for src, dst in pairs:
            made[name].append(
                functools.partial(
                    pltpu.make_async_remote_copy,
                    src_ref=src,
                    dst_ref=dst,
                    send_sem=send.at[slot],
                    recv_sem=recv.at[slot],
                    device_id={"bar": where[0], "lat": where[1]},
                    device_id_type=MESH,
                )
            )
            slot += 1
    return made


def kernel(
    bars,
    u_hbm, v_hbm, low_hbm, high_hbm, bc_hbm,
    base_out, half_out,
    frame, flags, vel, speeds, bc, turned, spun, weight, local, send, recv,
):
    bar, lat = lax.axis_index("bar"), lax.axis_index("lat")
    has_left, has_right = bar > 0, bar < bars - 1
    flat_frame = frame.reshape(STEPS, 3, PLANES * ROWS, NZ)
    flat_flags = flags.reshape(2, PLANES * ROWS, NZ)
    flat_vel = vel.reshape(3, PLANES * ROWS, NZ)
    flat_turned = turned.reshape(STEPS, 5, 3, PLANES * ROWS, NZ)
    flat_spun = spun.reshape(2, 5, PLANES * ROWS, NZ)

    loads = [
        pltpu.make_async_copy(low_hbm, flags.at[0, X0:X0 + CX, OWN], local.at[0]),
        pltpu.make_async_copy(high_hbm, flags.at[1, X0:X0 + CX, OWN], local.at[1]),
        pltpu.make_async_copy(u_hbm, frame.at[0, :, X0:X0 + CX, OWN], local.at[2]),
        pltpu.make_async_copy(v_hbm, vel.at[:, X0:X0 + CX, OWN], local.at[3]),
        pltpu.make_async_copy(bc_hbm, bc, local.at[4]),
    ]
    barrier = pltpu.get_barrier_semaphore()

    def greet(b, l):
        pl.semaphore_signal(barrier, inc=1, device_id={"bar": b, "lat": l}, device_id_type=MESH)

    greet(bar, 1 - lat)

    @pl.when(has_left)
    def _():
        greet(bar - 1, lat)
        greet(bar - 1, 1 - lat)

    @pl.when(has_right)
    def _():
        greet(bar + 1, lat)
        greet(bar + 1, 1 - lat)

    for copy in loads:
        copy.start()

    void = pl.ds(pl.multiple_of(lat * (2 * RY), RY), RY)
    halo = pl.ds(pl.multiple_of((1 - lat) * (2 * RY), RY), RY)
    for step, first, last in ((0, 1, 17), (1, 4, 14)):
        zero = jnp.zeros((last - first, RY, NZ), F32)
        for comp in range(3):
            if comp < 2:
                frame[step, comp, first:last, void, :] = zero
            for c in TURNS:
                turned[step, c + 2, comp, first:last, void, :] = zero
    for word in range(2):
        flags[word, 0:15, void, :] = jnp.full((15, RY, NZ), -1, jnp.int32)
        for c in TURNS:
            spun[word, c + 2, 1:15, void, :] = jnp.full((14, RY, NZ), -1, jnp.int32)

    @pl.when(jnp.logical_not(has_left))
    def _():
        for comp in range(3):
            frame[0, comp, 0:6] = jnp.zeros((6, ROWS, NZ), F32)
            vel[comp, 3:6] = jnp.zeros((3, ROWS, NZ), F32)
        for word in range(2):
            flags[word, 0:6] = jnp.full((6, ROWS, NZ), -1, jnp.int32)

    @pl.when(jnp.logical_not(has_right))
    def _():
        for comp in range(3):
            frame[0, comp, 12:18] = jnp.zeros((6, ROWS, NZ), F32)
            vel[comp, 12:15] = jnp.zeros((3, ROWS, NZ), F32)

    sems = (send, recv)
    refs = (frame.at[0], vel, flags)
    sent = copies(lat, refs, sems, bar, lat)
    got = copies(1 - lat, refs, sems, bar, lat)

    def exchange(names, act):
        for name in names:
            partner = name.removesuffix("_v")
            made = got if act == "wait_recv" and partner.startswith("over") else sent
            if act == "wait_recv":
                there = {"right": has_left, "left": has_right}.get(partner.split("_")[-1])
            else:
                there = {"right": has_right, "left": has_left}.get(partner.split("_")[-1])

            def run():
                for copy in made[name]:
                    getattr(copy(), act)()

            if there is None:
                run()
            else:
                pl.when(there)(run)

    row = lax.broadcasted_iota(jnp.int32, (RY, NZ), 0)
    lane = lax.broadcasted_iota(jnp.int32, (RY, NZ), 1)
    for copy in loads[:2]:
        copy.wait()
    for word in range(2):
        gone = jnp.zeros((RY, NZ), jnp.int32)
        for t in range(3):
            under = bits_where(lambda a, b, c: b < -t)[word]
            above = bits_where(lambda a, b, c: b > t)[word]
            cut = jnp.where(lat == 0, jnp.int32(under), jnp.int32(above))
            gone = jnp.where(row == t + lat * (RY - 1 - 2 * t), cut, gone)
        for t in range(3):
            under = bits_where(lambda a, b, c: c < -t)[word]
            above = bits_where(lambda a, b, c: c > t)[word]
            gone = jnp.where(lane == t, gone | jnp.int32(under), gone)
            gone = jnp.where(lane == NZ - 1 - t, gone | jnp.int32(above), gone)
        for x in range(CX):
            flags[word, X0 + x, OWN, :] = flags[word, X0 + x, OWN, :] | gone

    @pl.when(jnp.logical_not(has_right))
    def _():
        for x in range(3, CX):
            beyond = bits_where(lambda a, b, c: x + a >= CX)
            for word in range(2):
                flags[word, X0 + x, OWN, :] = flags[word, X0 + x, OWN, :] | jnp.int32(beyond[word])

    for copy in loads[2:]:
        copy.wait()
    sign = 1 - 2 * lat
    fsign = sign.astype(F32)
    edge_row = {d: Y0 + RY - 1 + d - lat * (RY - 1 + 2 * d) for d in (1, 2, 3)}

    class Tile:
        def __init__(self, plane):
            self.plane = plane

        def get(self, ref, flat, lead, a, b):
            return ref[(*lead, X0 + self.plane + a, pl.ds(Y0 + b, RY), slice(None))]

        def put(self, ref, flat, lead, value):
            ref[(*lead, X0 + self.plane, OWN, slice(None))] = value

    class Row:
        def __init__(self, plane, d):
            self.plane, self.d = plane, d

        def at(self, a, b):
            return pl.ds(edge_row[self.d] + ((X0 + self.plane + a) * ROWS + b), RY, stride=ROWS)

        def get(self, ref, flat, lead, a, b):
            return flat[(*lead, self.at(a, b), slice(None))]

        def put(self, ref, flat, lead, value):
            flat[(*lead, self.at(0, 0), slice(None))] = value

    def spin(plane, rows, words=(0, 1)):
        for word in words:
            held = flags[word, plane, rows, :]
            for c in TURNS:
                spun[word, c + 2, plane, rows, :] = pltpu.roll(held, (-c) % NZ, axis=1)

    def turn(step, plane, rows):
        for comp in range(3):
            held = frame[step, comp, plane, rows, :]
            for c in TURNS:
                moved = pltpu.roll(held, (-c) % NZ, axis=1)
                turned[step, c + 2, comp, plane, rows, :] = combine([(c if comp == 2 else 1, moved)])

    def put_weight(xi, back, planes):
        a, b, c = xi
        word, bit = flag_of(xi)
        a1, b1, c1 = (-a, -b, -c) if back else xi
        place = PLACE[abs(b1)][(a1, c1)]
        for x in planes:
            if not back:
                held = flags[word, X0 + x, OWN, :]
            elif c == 0:
                held = flags[word, X0 + x + a1, Y0 + b1:Y0 + b1 + RY, :]
            elif c == 3:
                held = pltpu.roll(flags[word, X0 + x, OWN, :], 3, axis=1)
            else:
                held = spun[word, c1 + 2, X0 + x + a1, Y0 + b1:Y0 + b1 + RY, :]
            weight[b1 + 3, place, x] = jnp.where((held & jnp.int32(bit)) == 0, F32(strength(*xi)), F32(0.0))

    def add_terms(step, b, shift, factor, c, tasks):
        seen = {}
        for group, todo, force, want, table in tasks:
            if 0 not in want:
                todo = todo if (b or c) and (1 not in want or b or 2 in want) else []
            elif want == (0,):
                todo = [a for a in todo if a]
            todo = [a for a in todo if a or b or c]
            if not todo:
                continue

            def fetch(comp, a):
                if c == 0:
                    return group.get(frame, flat_frame, (step, comp), a, shift)
                return group.get(turned, flat_turned, (step, c + 2, comp), a, shift)

            def mine(comp):
                return group.get(frame, flat_frame, (step, comp), 0, 0)

            def nearby(a):
                key = (group.plane + a, isinstance(group, Row) and group.d)
                if key not in seen:
                    terms = []
                    if abs(c) == 3:
                        terms.append((c, pltpu.roll(mine(2), (-c) % NZ, axis=1)))
                    elif c:
                        terms.append((1, fetch(2, a)))
                    if b:
                        terms.append((factor, fetch(1, a)))
                    seen[key] = combine(terms)
                return seen[key]

            def kept(a, value):
                if table is not None:
                    return table[PLACE[abs(b)][(a, c)], group.plane] * value
                if (a, b, c) in NUMBER:
                    word, bit = flag_of((a, b, c))
                    held = group.get(flags, flat_flags, (word,), 0, 0)
                else:
                    word, bit = flag_of((-a, -b, -c))
                    if c == 0:
                        held = group.get(flags, flat_flags, (word,), a, b)
                    elif c == -3:
                        held = pltpu.roll(group.get(flags, flat_flags, (word,), 0, 0), 3, axis=1)
                    else:
                        held = group.get(spun, flat_spun, (word, c + 2), a, b)
                return jnp.where((held & jnp.int32(bit)) == 0, value, F32(0.0))

            mine0 = mine(0) if any(todo) else None
            base = combine([(factor, mine(1))] * bool(b) + [(c, mine(2))] * bool(c))
            pulls = {}
            for a in todo:
                if base is None:
                    pulls[a] = kept(a, fetch(0, a) - mine0)
                    continue
                there, here = nearby(a), base
                if a:
                    there = combine([(1, there), (a, fetch(0, a))])
                    here = combine([(1, here), (a, mine0)])
                pulls[a] = kept(a, there - here)
            total, along = None, None
            for size in range(4):
                plus, minus = pulls.get(size), pulls.get(-size) if size else None
                if plus is None and minus is None:
                    continue
                k = 1.0 if table is not None else strength(size, b, c)
                if base is None:
                    both = combine([(1, v) for v in (plus, minus) if v is not None])
                    along = combine([(1, along)] * (along is not None) + [(k * size * size, both)])
                    continue
                both = combine([(1, v) for v in (plus, minus) if v is not None])
                total = combine([(1, total)] * (total is not None) + [(k, both)])
                if size and 0 in want:
                    if plus is None:
                        term = (-k * size, minus)
                    elif minus is None:
                        term = (k * size, plus)
                    else:
                        term = (k * size, plus - minus)
                    along = combine([(1, along)] * (along is not None) + [term])
            for comp, k, value in ((0, 1, along), (1, factor, total), (2, c, total)):
                if comp not in want or value is None or (comp == 1 and not b) or (comp == 2 and not c):
                    continue
                force[comp] = combine([(1, force[comp])] * (force[comp] is not None) + [(k, value)])

    retain = {}
    for key, where in (("left", jnp.maximum(bar - 1, 0)), ("own", bar), ("right", jnp.minimum(bar + 1, bars - 1))):
        retain[key] = 1.0 - 0.2 * bc[where].astype(F32)

    def retain_of(group):
        if isinstance(group, Tile):
            return retain["left" if group.plane < 0 else "own" if group.plane < CX else "right"]
        plane = row + group.plane
        return jnp.where(plane < 0, retain["left"], jnp.where(plane < CX, retain["own"], retain["right"]))

    def advance(group, force, want=(0, 1, 2)):
        keep = retain_of(group)
        for comp in want:
            speed = keep * (group.get(vel, flat_vel, (comp,), 0, 0) + force[comp])
            moved = group.get(frame, flat_frame, (0, comp), 0, 0) + F32(time_step) * speed
            if isinstance(group, Tile) and 0 <= group.plane < CX:
                speeds[comp, group.plane] = speed
            group.put(frame, flat_frame, (1, comp), moved)
            far = (group.plane in (-3, 8)) if isinstance(group, Tile) else group.d == 3
            if not far:
                for c in TURNS:
                    value = pltpu.roll(moved, (-c) % NZ, axis=1)
                    group.put(turned, flat_turned, (1, c + 2, comp), combine([(c if comp == 2 else 1, value)]))

    def blank():
        return [None, None, None]

    def span(b, c):
        far = reach(b, c)
        return range(-far, far + 1)

    own = [Tile(x) for x in range(CX)]
    force = [blank() for _ in range(CX)]
    every = (0, 1, 2)

    def own_terms(step, beta, c, chosen, pulls):
        shift, factor = (sign * beta, fsign * F32(beta)) if beta else (0, 0)
        table = weight.at[3 + shift]
        tasks = [
            (own[x], [a for a in span(beta, c) if chosen(x, x + a)], pulls[x], every, table) for x in range(CX)
        ]
        add_terms(step, beta, shift, factor, c, tasks)

    def outer(groups_wants, chosen=lambda group, a: True):
        made = [(entry[0], entry[2] if len(entry) > 2 else blank(), entry[1]) for entry in groups_wants]
        for b, c in PAIRS:
            add_terms(
                0, b, b, b, c,
                [(group, [a for a in span(b, c) if chosen(group, a)], pull, want, None) for group, pull, want in made],
            )
        return made

    def advance_all(made):
        for group, pull, want in made:
            advance(group, pull, want)

    for x in range(CX):
        spin(X0 + x, OWN)
        turn(0, X0 + x, OWN)
    for xi in BONDS:
        put_weight(xi, False, range(CX))
    for xi in BONDS:
        if xi[1] == 0:
            put_weight(xi, True, range(xi[0], CX))
    for side in range(2):

        @pl.when(lat == side)
        def _():
            for xi in BONDS:
                if xi[1] * (1 - 2 * side) > 0:
                    put_weight(xi, True, range(xi[0], CX))

    for beta, c in PAIRS:
        if beta <= 0:
            own_terms(0, beta, c, lambda x, q: 0 <= q < CX, force)

    pl.semaphore_wait(barrier, 1 + 2 * has_left.astype(jnp.int32) + 2 * has_right.astype(jnp.int32))
    exchange(tuple(sent), "start")

    exchange(("left", "over_left"), "wait_recv")
    for plane in range(12, 17):
        turn(0, plane, OWN)
        turn(0, plane, halo)
    for plane in range(12, 15):
        spin(plane, OWN)
        spin(plane, halo)
    for b, c in PAIRS:
        add_terms(0, b, b, b, c, [
            (own[x], [a for a in span(b, c) if x + a >= CX], force[x], every, weight.at[3 + b]) for x in range(CX)
        ])
    right_tiles = [(Tile(6), every, blank()), (Tile(7), every, blank()), (Tile(8), (0,), blank())]
    right_rows = [(Row(6, d), every, blank()) for d in (1, 2)]
    outer(right_tiles, lambda group, a: group.plane + a >= CX)
    for entry in right_rows:
        outer([entry], lambda group, a: a >= 0)

    exchange(("over",), "wait_recv")
    for x in range(CX):
        spin(X0 + x, halo)
        turn(0, X0 + x, halo)
    for side in range(2):

        @pl.when(lat == side)
        def _():
            for xi in BONDS:
                if xi[1] * (1 - 2 * side) < 0:
                    put_weight(xi, True, range(xi[0], CX))

    for beta, c in PAIRS:
        if beta > 0:
            own_terms(0, beta, c, lambda x, q: 0 <= q < CX, force)
    for x in range(3, CX):
        advance(own[x], force[x])
    made = outer(right_tiles, lambda group, a: group.plane + a < CX)
    exchange(("left_v",), "wait_recv")
    advance_all(made)
    made = []
    for entry in right_rows:
        made += outer([entry], lambda group, a: a < 0)
    exchange(("over_v", "over_left_v"), "wait_recv")
    advance_all(made)
    third = blank()
    outer([(Row(0, 3), (1,), third)], lambda group, a: a >= 0)
    again = [blank() for _ in range(CX)]

    def early(x, q):
        return x >= 3 and q >= 3

    for beta, c in PAIRS:
        if beta <= 0:
            own_terms(1, beta, c, early, again)

    exchange(("right", "over_right"), "wait_recv")
    for plane in range(1, 6):
        spin(plane, OWN)
        turn(0, plane, OWN)
        spin(plane, halo)
        turn(0, plane, halo)
    for xi in BONDS:
        put_weight(xi, True, range(min(xi[0], CX)))
    for beta, c in PAIRS:
        own_terms(0, beta, c, lambda x, q: q < 0, force)
    for x in range(3):
        advance(own[x], force[x])
    made = outer([(Tile(-3), (0,)), (Tile(-2), every), (Tile(-1), every)])
    exchange(("right_v", "over_right_v"), "wait_recv")
    advance_all(made)
    made = outer([(Row(-2, 1), every)]) + outer([(Row(-2, 2), every)])
    made += outer([(Row(0, 3), (1,), third)], lambda group, a: a < 0)
    advance_all(made)

    for beta, c in PAIRS:
        own_terms(1, beta, c, (lambda x, q: not early(x, q)) if beta <= 0 else (lambda x, q: True), again)
    for x in range(CX):
        for comp in range(3):
            speed = retain["own"] * (speeds[comp, x] + again[x][comp])
            half_out[comp, x] = F32(time_step) * speed
            base_out[comp, x] = frame[1, comp, X0 + x, OWN, :]
    exchange(tuple(sent), "wait_send")


def local_steps(bars, displace, velocity, bond_low, bond_high, bc_type):
    any_space = pl.BlockSpec(memory_space=pl.ANY)
    out = pltpu.VMEM(displace.shape, F32)
    base, half = pl.pallas_call(
        functools.partial(kernel, bars),
        out_shape=(out, out),
        in_specs=[any_space] * 5,
        scratch_shapes=[
            pltpu.VMEM((STEPS, 3, PLANES, ROWS, NZ), F32),
            pltpu.VMEM((2, PLANES, ROWS, NZ), jnp.int32),
            pltpu.VMEM((3, PLANES, ROWS, NZ), F32),
            pltpu.VMEM((3, CX, RY, NZ), F32),
            pltpu.SMEM((bc_type.shape[0],), jnp.int32),
            pltpu.VMEM((STEPS, 5, 3, PLANES, ROWS, NZ), F32),
            pltpu.VMEM((2, 5, PLANES, ROWS, NZ), jnp.int32),
            pltpu.VMEM((7, 29, CX, RY, NZ), F32),
            pltpu.SemaphoreType.DMA((5,)),
            pltpu.SemaphoreType.DMA((20,)),
            pltpu.SemaphoreType.DMA((20,)),
        ],
        compiler_params=pltpu.CompilerParams(collective_id=0, has_side_effects=True),
        name="peridynamics",
    )(displace, velocity, bond_low, bond_high, bc_type)
    return base + half, half + half


def solution(mesh):
    bars = mesh.shape["bar"]
    return jax.shard_map(
        functools.partial(local_steps, bars),
        mesh=mesh,
        in_specs=(
            P(None, "bar", "lat", None),
            P(None, "bar", "lat", None),
            P("bar", "lat", None),
            P("bar", "lat", None),
            P(),
        ),
        out_specs=(P(None, "bar", "lat", None), P(None, "bar", "lat", None)),
        check_vma=False,
    )
```

```python
import functools

import jax
import jax.numpy as jnp
from jax import lax
from jax.experimental import pallas as pl
from jax.experimental.pallas import tpu as pltpu
from jax.sharding import PartitionSpec as P

STEPS = 2
modulus = 0.1
time_step = 0.5
MESH = pl.DeviceIdType.MESH

CX, RY, NZ = 6, 8, 128
PLANES, ROWS = 3 * CX + 5, 3 * RY
X0, Y0 = CX, RY
LINE = 25
OWN = slice(Y0, Y0 + RY)
F32 = jnp.float32


def bond_offsets():
    found = []
    for a in range(-3, 4):
        for b in range(-3, 4):
            for c in range(-3, 4):
                square = a * a + b * b + c * c
                if square == 0 or square > 9:
                    continue
                if a > 0 or (a == 0 and b > 0) or (a == 0 and b == 0 and c > 0):
                    found.append((a, b, c))
    return found


BONDS = bond_offsets()
NUMBER = {xi: k for k, xi in enumerate(BONDS)}
TURNS = (-2, -1, 1, 2)


def flag_of(xi):
    k = NUMBER[xi]
    return (0, 1 << k) if k < 31 else (1, 1 << (k - 31))


def bits_where(test):
    words = [0, 0]
    for xi in BONDS:
        if test(*xi):
            word, bit = flag_of(xi)
            words[word] |= bit
    return words


def disc(b):
    return [(a, c) for c in range(-3, 4) for a in range(-3, 4) if a * a + b * b + c * c <= 9]


PLACE = {abs(b): {ac: n for n, ac in enumerate(disc(b))} for b in range(4)}
PAIRS = [
    pair
    for c in range(0, 4)
    for b in range(-3, 4)
    if b * b + c * c <= 9 and (c > 0 or b >= 0)
    for pair in dict.fromkeys(((b, c), (-b, -c)))
]


def reach(b, c):
    return max(a for a in range(4) if a * a + b * b + c * c <= 9)


def strength(a, b, c):
    return time_step * (modulus / float(a * a + b * b + c * c) ** 1.5)


def combine(terms):
    terms = sorted(terms, key=lambda kv: isinstance(kv[0], (int, float)) and kv[0] < 0)
    out = None
    for k, v in terms:
        if not isinstance(k, (int, float)):
            out = v * k if out is None else out + v * k
            continue
        if k == 0:
            continue
        w = v if abs(k) == 1 else v * F32(abs(k))
        if out is None:
            out = w if k > 0 else -w
        else:
            out = out + w if k > 0 else out - w
    return out


def copies(side, refs, sems, bar, lat):
    u, v, flags = refs
    send, recv = sems

    def rows(ref, lead, src, dst, n):
        here = pl.ds(2 * RY - n - side * (RY - n), n)
        there = pl.ds(RY - n + side * (RY + n), n)
        return ref.at[lead, src, here], ref.at[lead, dst, there]

    def tile(ref, lead, src, dst):
        return ref.at[lead, src, OWN], ref.at[lead, dst, OWN]

    every = slice(None)
    own = slice(6, 12)
    plan = {
        "over_right": [
            rows(u, every, slice(7, 12), slice(1, 6), 5),
            rows(flags, every, slice(7, 12), slice(1, 6), 5),
        ],
        "right": [
            tile(u, every, slice(7, 12), slice(1, 6)),
            tile(flags, 1, own, slice(0, 6)),
            tile(flags, 0, slice(8, 12), slice(2, 6)),
            tile(u, 0, slice(6, 7), slice(0, 1)),
        ],
        "over_left": [
            rows(u, every, slice(6, 11), slice(12, 17), 5),
            rows(flags, every, slice(6, 9), slice(12, 15), 5),
        ],
        "left": [
            tile(u, every, slice(6, 11), slice(12, 17)),
            tile(flags, every, slice(6, 9), slice(12, 15)),
            tile(u, 0, slice(11, 12), slice(17, 18)),
        ],
        "over": [rows(u, every, own, own, 6), rows(flags, every, own, own, 6)],
        "over_right_v": [rows(v, every, slice(10, 12), slice(4, 6), 2)],
        "right_v": [tile(v, every, slice(10, 12), slice(4, 6)), tile(v, 0, slice(9, 10), slice(3, 4))],
        "over_left_v": [rows(v, every, slice(6, 8), slice(12, 14), 2)],
        "left_v": [tile(v, every, slice(6, 8), slice(12, 14)), tile(v, 0, slice(8, 9), slice(14, 15))],
        "over_v": [rows(v, every, own, own, 3)],
    }
    partner = {
        "right": (bar + 1, lat),
        "left": (bar - 1, lat),
        "over": (bar, 1 - lat),
        "over_right": (bar + 1, 1 - lat),
        "over_left": (bar - 1, 1 - lat),
    }
    made = {}
    slot = 0
    for name, pairs in plan.items():
        made[name] = []
        where = partner[name.removesuffix("_v")]
        for src, dst in pairs:
            made[name].append(
                functools.partial(
                    pltpu.make_async_remote_copy,
                    src_ref=src,
                    dst_ref=dst,
                    send_sem=send.at[slot],
                    recv_sem=recv.at[slot],
                    device_id={"bar": where[0], "lat": where[1]},
                    device_id_type=MESH,
                )
            )
            slot += 1
    return made


def kernel(
    bars,
    u_hbm, v_hbm, low_hbm, high_hbm, bc_hbm,
    base_out, half_out,
    frame, flags, vel, speeds, bc, lines, marks, turned, spun, weight, local, send, recv,
):
    bar, lat = lax.axis_index("bar"), lax.axis_index("lat")
    has_left, has_right = bar > 0, bar < bars - 1
    flat_frame = frame.reshape(STEPS, 3, PLANES * ROWS, NZ)
    flat_vel = vel.reshape(3, PLANES * ROWS, NZ)
    flat_turned = turned.reshape(STEPS, 5, 3, PLANES * ROWS, NZ)

    loads = [
        pltpu.make_async_copy(low_hbm, flags.at[0, X0:X0 + CX, OWN], local.at[0]),
        pltpu.make_async_copy(high_hbm, flags.at[1, X0:X0 + CX, OWN], local.at[1]),
        pltpu.make_async_copy(u_hbm, frame.at[0, :, X0:X0 + CX, OWN], local.at[2]),
        pltpu.make_async_copy(v_hbm, vel.at[:, X0:X0 + CX, OWN], local.at[3]),
        pltpu.make_async_copy(bc_hbm, bc, local.at[4]),
    ]
    barrier = pltpu.get_barrier_semaphore()

    def greet(b, l):
        pl.semaphore_signal(barrier, inc=1, device_id={"bar": b, "lat": l}, device_id_type=MESH)

    greet(bar, 1 - lat)

    @pl.when(has_left)
    def _():
        greet(bar - 1, lat)
        greet(bar - 1, 1 - lat)

    @pl.when(has_right)
    def _():
        greet(bar + 1, lat)
        greet(bar + 1, 1 - lat)

    for copy in loads:
        copy.start()

    void = pl.ds(pl.multiple_of(lat * (2 * RY), RY), RY)
    halo_start = pl.multiple_of((1 - lat) * (2 * RY), RY)
    halo = pl.ds(halo_start, RY)
    for step, first, last in ((0, 1, 17), (1, 4, 14)):
        zero = jnp.zeros((last - first, RY, NZ), F32)
        for comp in range(3):
            if comp < 2:
                frame[step, comp, first:last, void, :] = zero
            for c in TURNS:
                turned[step, c + 2, comp, first:last, void, :] = zero
    for word in range(2):
        flags[word, 0:15, void, :] = jnp.full((15, RY, NZ), -1, jnp.int32)
        for c in TURNS:
            spun[word, c + 2, 1:15, void, :] = jnp.full((14, RY, NZ), -1, jnp.int32)

    @pl.when(jnp.logical_not(has_left))
    def _():
        for comp in range(3):
            frame[0, comp, 0:6] = jnp.zeros((6, ROWS, NZ), F32)
            vel[comp, 3:6] = jnp.zeros((3, ROWS, NZ), F32)
        for word in range(2):
            flags[word, 0:6] = jnp.full((6, ROWS, NZ), -1, jnp.int32)

    @pl.when(jnp.logical_not(has_right))
    def _():
        for comp in range(3):
            frame[0, comp, 12:18] = jnp.zeros((6, ROWS, NZ), F32)
            vel[comp, 12:15] = jnp.zeros((3, ROWS, NZ), F32)

    sems = (send, recv)
    refs = (frame.at[0], vel, flags)
    sent = copies(lat, refs, sems, bar, lat)
    got = copies(1 - lat, refs, sems, bar, lat)

    def exchange(names, act):
        for name in names:
            partner = name.removesuffix("_v")
            made = got if act == "wait_recv" and partner.startswith("over") else sent
            if act == "wait_recv":
                there = {"right": has_left, "left": has_right}.get(partner.split("_")[-1])
            else:
                there = {"right": has_right, "left": has_left}.get(partner.split("_")[-1])

            def run():
                for copy in made[name]:
                    getattr(copy(), act)()

            if there is None:
                run()
            else:
                pl.when(there)(run)

    row = lax.broadcasted_iota(jnp.int32, (RY, NZ), 0)
    lane = lax.broadcasted_iota(jnp.int32, (RY, NZ), 1)
    for copy in loads[:2]:
        copy.wait()
    for word in range(2):
        gone = jnp.zeros((RY, NZ), jnp.int32)
        for t in range(3):
            under = bits_where(lambda a, b, c: b < -t)[word]
            above = bits_where(lambda a, b, c: b > t)[word]
            cut = jnp.where(lat == 0, jnp.int32(under), jnp.int32(above))
            gone = jnp.where(row == t + lat * (RY - 1 - 2 * t), cut, gone)
        for t in range(3):
            under = bits_where(lambda a, b, c: c < -t)[word]
            above = bits_where(lambda a, b, c: c > t)[word]
            gone = jnp.where(lane == t, gone | jnp.int32(under), gone)
            gone = jnp.where(lane == NZ - 1 - t, gone | jnp.int32(above), gone)
        for x in range(CX):
            flags[word, X0 + x, OWN, :] = flags[word, X0 + x, OWN, :] | gone

    @pl.when(jnp.logical_not(has_right))
    def _():
        for x in range(3, CX):
            beyond = bits_where(lambda a, b, c: x + a >= CX)
            for word in range(2):
                flags[word, X0 + x, OWN, :] = flags[word, X0 + x, OWN, :] | jnp.int32(beyond[word])

    for copy in loads[2:]:
        copy.wait()
    sign = 1 - 2 * lat
    fsign = sign.astype(F32)
    edge_row = {d: Y0 + RY - 1 + d - lat * (RY - 1 + 2 * d) for d in (1, 2, 3)}

    class Tile:
        def __init__(self, plane):
            self.plane = plane

        def get(self, ref, lead, a, b):
            return ref[(*lead, X0 + self.plane + a, pl.ds(Y0 + b, RY), slice(None))]

        def put(self, ref, flat, lead, value):
            ref[(*lead, X0 + self.plane, OWN, slice(None))] = value

    class Row:
        def __init__(self, plane, d):
            self.plane, self.d = plane, d

        def get(self, ref, lead, a, b):
            at = pl.ds(edge_row[self.d] * LINE + ((X0 + self.plane + a) + b * LINE), RY)
            if ref is frame:
                return lines[2, lead[1], at, :]
            if ref is turned:
                return lines[lead[1], lead[2], at, :]
            if ref is flags:
                return marks[lead[0], 2, at, :]
            if ref is spun:
                return marks[lead[0], lead[1], at, :]
            return flat_vel[(*lead, self.strided(), slice(None))]

        def strided(self):
            return pl.ds(edge_row[self.d] + (X0 + self.plane) * ROWS, RY, stride=ROWS)

        def put(self, ref, flat, lead, value):
            flat[(*lead, self.strided(), slice(None))] = value

    def line(plane, rows):
        return pl.ds((Y0 * LINE if rows is OWN else halo_start * LINE) + plane, RY, stride=LINE)

    def spin(plane, rows, turns=(-2, -1, 0, 1, 2)):
        for word in range(2):
            held = flags[word, plane, rows, :]
            for c in turns:
                moved = pltpu.roll(held, (-c) % NZ, axis=1) if c else held
                marks[word, c + 2, line(plane, rows), :] = moved
                if c:
                    spun[word, c + 2, plane, rows, :] = moved

    def turn(plane, rows, turns=(-2, -1, 0, 1, 2)):
        for comp in range(3):
            held = frame[0, comp, plane, rows, :]
            for c in turns:
                moved = combine([(c if comp == 2 else 1, pltpu.roll(held, (-c) % NZ, axis=1))]) if c else held
                lines[c + 2, comp, line(plane, rows), :] = moved
                if c:
                    turned[0, c + 2, comp, plane, rows, :] = moved

    def put_weight(xi, back, planes):
        a, b, c = xi
        word, bit = flag_of(xi)
        a1, b1, c1 = (-a, -b, -c) if back else xi
        place = PLACE[abs(b1)][(a1, c1)]
        for x in planes:
            if not back:
                held = flags[word, X0 + x, OWN, :]
            elif c == 0:
                held = flags[word, X0 + x + a1, Y0 + b1:Y0 + b1 + RY, :]
            elif c == 3:
                held = pltpu.roll(flags[word, X0 + x, OWN, :], 3, axis=1)
            else:
                held = spun[word, c1 + 2, X0 + x + a1, Y0 + b1:Y0 + b1 + RY, :]
            weight[b1 + 3, place, x] = jnp.where((held & jnp.int32(bit)) == 0, F32(strength(*xi)), F32(0.0))

    heres = {}

    def add_terms(step, b, shift, factor, c, tasks):
        seen = {}
        opposite = (step, -b, -c)
        for key in list(heres):
            if key[:3] != opposite:
                del heres[key]
        for group, todo, force, want, table in tasks:
            if 0 not in want:
                todo = todo if (b or c) and (1 not in want or b or 2 in want) else []
            elif want == (0,):
                todo = [a for a in todo if a]
            todo = [a for a in todo if a or b or c]
            if not todo:
                continue

            def fetch(comp, a):
                if c == 0:
                    return group.get(frame, (step, comp), a, shift)
                return group.get(turned, (step, c + 2, comp), a, shift)

            def mine(comp):
                return group.get(frame, (step, comp), 0, 0)

            def nearby(a):
                key = (group.plane + a, isinstance(group, Row) and group.d)
                if key not in seen:
                    terms = []
                    if abs(c) == 3:
                        terms.append((c, pltpu.roll(mine(2), (-c) % NZ, axis=1)))
                    elif c:
                        terms.append((1, fetch(2, a)))
                    if b:
                        terms.append((factor, fetch(1, a)))
                    seen[key] = combine(terms)
                return seen[key]

            def kept(a, value):
                if table is not None:
                    return table[PLACE[abs(b)][(a, c)], group.plane] * value
                if (a, b, c) in NUMBER:
                    word, bit = flag_of((a, b, c))
                    held = group.get(flags, (word,), 0, 0)
                else:
                    word, bit = flag_of((-a, -b, -c))
                    if c == 0:
                        held = group.get(flags, (word,), a, b)
                    elif c == -3:
                        held = pltpu.roll(group.get(flags, (word,), 0, 0), 3, axis=1)
                    else:
                        held = group.get(spun, (word, c + 2), a, b)
                return jnp.where((held & jnp.int32(bit)) == 0, value, F32(0.0))

            needs = [a for a in todo if (*opposite, -a, group) not in heres]
            mine0 = mine(0) if any(needs) else None
            alone = not b and not c
            base = combine([(factor, mine(1))] * bool(b) + [(c, mine(2))] * bool(c)) if needs else None
            pulls = {}
            for a in todo:
                if alone:
                    pulls[a] = kept(a, fetch(0, a) - mine0)
                    continue
                there = nearby(a)
                if a:
                    there = combine([(1, there), (a, fetch(0, a))])
                if a in needs:
                    here = combine([(1, base), (a, mine0)]) if a else base
                    heres[(step, b, c, a, group)] = here
                    pulls[a] = kept(a, there - here)
                else:
                    pulls[a] = kept(a, there + heres[(*opposite, -a, group)])
            total, along = None, None
            for size in range(4):
                plus, minus = pulls.get(size), pulls.get(-size) if size else None
                if plus is None and minus is None:
                    continue
                k = 1.0 if table is not None else strength(size, b, c)
                if alone:
                    both = combine([(1, v) for v in (plus, minus) if v is not None])
                    along = combine([(1, along)] * (along is not None) + [(k * size * size, both)])
                    continue
                both = combine([(1, v) for v in (plus, minus) if v is not None])
                total = combine([(1, total)] * (total is not None) + [(k, both)])
                if size and 0 in want:
                    if plus is None:
                        term = (-k * size, minus)
                    elif minus is None:
                        term = (k * size, plus)
                    else:
                        term = (k * size, plus - minus)
                    along = combine([(1, along)] * (along is not None) + [term])
            for comp, k, value in ((0, 1, along), (1, factor, total), (2, c, total)):
                if comp not in want or value is None or (comp == 1 and not b) or (comp == 2 and not c):
                    continue
                force[comp] = combine([(1, force[comp])] * (force[comp] is not None) + [(k, value)])

    retain = {}
    for key, where in (("left", jnp.maximum(bar - 1, 0)), ("own", bar), ("right", jnp.minimum(bar + 1, bars - 1))):
        retain[key] = 1.0 - 0.2 * bc[where].astype(F32)

    def retain_of(group):
        if isinstance(group, Tile):
            return retain["left" if group.plane < 0 else "own" if group.plane < CX else "right"]
        plane = row + group.plane
        return jnp.where(plane < 0, retain["left"], jnp.where(plane < CX, retain["own"], retain["right"]))

    def advance(group, force, want=(0, 1, 2)):
        keep = retain_of(group)
        for comp in want:
            speed = keep * (group.get(vel, (comp,), 0, 0) + force[comp])
            moved = group.get(frame, (0, comp), 0, 0) + F32(time_step) * speed
            if isinstance(group, Tile) and 0 <= group.plane < CX:
                speeds[comp, group.plane] = speed
            group.put(frame, flat_frame, (1, comp), moved)
            far = (group.plane in (-3, 8)) if isinstance(group, Tile) else group.d == 3
            if not far:
                for c in TURNS:
                    value = pltpu.roll(moved, (-c) % NZ, axis=1)
                    group.put(turned, flat_turned, (1, c + 2, comp), combine([(c if comp == 2 else 1, value)]))

    def blank():
        return [None, None, None]

    def span(b, c):
        far = reach(b, c)
        return range(-far, far + 1)

    own = [Tile(x) for x in range(CX)]
    force = [blank() for _ in range(CX)]
    every = (0, 1, 2)

    def own_terms(step, beta, c, chosen, pulls):
        shift, factor = (sign * beta, fsign * F32(beta)) if beta else (0, 0)
        table = weight.at[3 + shift]
        tasks = [
            (own[x], [a for a in span(beta, c) if chosen(x, x + a)], pulls[x], every, table) for x in range(CX)
        ]
        add_terms(step, beta, shift, factor, c, tasks)

    def outer(groups_wants, chosen=lambda group, a: True):
        made = [(entry[0], entry[2] if len(entry) > 2 else blank(), entry[1]) for entry in groups_wants]
        for b, c in PAIRS:
            add_terms(
                0, b, b, b, c,
                [(group, [a for a in span(b, c) if chosen(group, a)], pull, want, None) for group, pull, want in made],
            )
        return made

    def advance_all(made):
        for group, pull, want in made:
            advance(group, pull, want)

    pl.semaphore_wait(barrier, 1 + 2 * has_left.astype(jnp.int32) + 2 * has_right.astype(jnp.int32))
    exchange(tuple(sent), "start")

    for x in range(CX):
        spin(X0 + x, OWN)
        turn(X0 + x, OWN)
    for xi in BONDS:
        put_weight(xi, False, range(CX))
    for xi in BONDS:
        if xi[1] == 0:
            put_weight(xi, True, range(xi[0], CX))
    for side in range(2):

        @pl.when(lat == side)
        def _():
            for xi in BONDS:
                if xi[1] * (1 - 2 * side) > 0:
                    put_weight(xi, True, range(xi[0], CX))

    for beta, c in PAIRS:
        if beta <= 0:
            own_terms(0, beta, c, lambda x, q: 0 <= q < CX, force)

    exchange(("left", "over_left"), "wait_recv")
    for plane in range(12, 17):
        turn(plane, OWN)
        turn(plane, halo)
    for plane in range(12, 15):
        spin(plane, OWN)
        spin(plane, halo)
    for b, c in PAIRS:
        add_terms(0, b, b, b, c, [
            (own[x], [a for a in span(b, c) if x + a >= CX], force[x], every, weight.at[3 + b]) for x in range(CX)
        ])
    right_tiles = [(Tile(6), every, blank()), (Tile(7), every, blank()), (Tile(8), (0,), blank())]
    right_rows = [(Row(6, d), every, blank()) for d in (1, 2)]
    outer(right_tiles, lambda group, a: group.plane + a >= CX)
    for entry in right_rows:
        outer([entry], lambda group, a: a >= 0)

    exchange(("over",), "wait_recv")
    for x in range(CX):
        spin(X0 + x, halo)
        turn(X0 + x, halo)
    for side in range(2):

        @pl.when(lat == side)
        def _():
            for xi in BONDS:
                if xi[1] * (1 - 2 * side) < 0:
                    put_weight(xi, True, range(xi[0], CX))

    for beta, c in PAIRS:
        if beta > 0:
            own_terms(0, beta, c, lambda x, q: 0 <= q < CX, force)
    for x in range(3, CX):
        advance(own[x], force[x])
    made = outer(right_tiles, lambda group, a: group.plane + a < CX)
    exchange(("left_v",), "wait_recv")
    advance_all(made)
    made = []
    for entry in right_rows:
        made += outer([entry], lambda group, a: a < 0)
    exchange(("over_v", "over_left_v"), "wait_recv")
    advance_all(made)
    third = blank()
    outer([(Row(0, 3), (1,), third)], lambda group, a: a >= 0)
    again = [blank() for _ in range(CX)]

    def early(x, q):
        return x >= 3 and q >= 3

    for beta, c in PAIRS:
        if beta <= 0:
            own_terms(1, beta, c, early, again)

    exchange(tuple(sent), "wait_send")
    exchange(("right", "over_right"), "wait_recv")
    for plane in range(1, 6):
        spin(plane, OWN)
        turn(plane, OWN)
        spin(plane, halo)
        turn(plane, halo)
    for xi in BONDS:
        put_weight(xi, True, range(min(xi[0], CX)))
    for beta, c in PAIRS:
        own_terms(0, beta, c, lambda x, q: q < 0, force)
    for x in range(3):
        advance(own[x], force[x])
    made = outer([(Tile(-3), (0,)), (Tile(-2), every), (Tile(-1), every)])
    exchange(("right_v", "over_right_v"), "wait_recv")
    advance_all(made)
    made = outer([(Row(-2, 1), every)]) + outer([(Row(-2, 2), every)])
    made += outer([(Row(0, 3), (1,), third)], lambda group, a: a < 0)
    advance_all(made)

    for beta, c in PAIRS:
        own_terms(1, beta, c, (lambda x, q: not early(x, q)) if beta <= 0 else (lambda x, q: True), again)
    for x in range(CX):
        for comp in range(3):
            speed = retain["own"] * (speeds[comp, x] + again[x][comp])
            half_out[comp, x] = F32(time_step) * speed
            base_out[comp, x] = frame[1, comp, X0 + x, OWN, :]


def local_steps(bars, displace, velocity, bond_low, bond_high, bc_type):
    any_space = pl.BlockSpec(memory_space=pl.ANY)
    out = pltpu.VMEM(displace.shape, F32)
    base, half = pl.pallas_call(
        functools.partial(kernel, bars),
        out_shape=(out, out),
        in_specs=[any_space] * 5,
        scratch_shapes=[
            pltpu.VMEM((STEPS, 3, PLANES, ROWS, NZ), F32),
            pltpu.VMEM((2, PLANES, ROWS, NZ), jnp.int32),
            pltpu.VMEM((3, PLANES, ROWS, NZ), F32),
            pltpu.VMEM((3, CX, RY, NZ), F32),
            pltpu.SMEM((bc_type.shape[0],), jnp.int32),
            pltpu.VMEM((5, 3, ROWS * LINE, NZ), F32),
            pltpu.VMEM((2, 5, ROWS * LINE, NZ), jnp.int32),
            pltpu.VMEM((STEPS, 5, 3, PLANES, ROWS, NZ), F32),
            pltpu.VMEM((2, 5, PLANES, ROWS, NZ), jnp.int32),
            pltpu.VMEM((7, 29, CX, RY, NZ), F32),
            pltpu.SemaphoreType.DMA((5,)),
            pltpu.SemaphoreType.DMA((20,)),
            pltpu.SemaphoreType.DMA((20,)),
        ],
        compiler_params=pltpu.CompilerParams(collective_id=0, has_side_effects=True),
        name="peridynamics",
    )(displace, velocity, bond_low, bond_high, bc_type)
    return base + half, half + half


def solution(mesh):
    bars = mesh.shape["bar"]
    return jax.shard_map(
        functools.partial(local_steps, bars),
        mesh=mesh,
        in_specs=(
            P(None, "bar", "lat", None),
            P(None, "bar", "lat", None),
            P("bar", "lat", None),
            P("bar", "lat", None),
            P(),
        ),
        out_specs=(P(None, "bar", "lat", None), P(None, "bar", "lat", None)),
        check_vma=False,
    )
```

```python
import functools

import jax
import jax.numpy as jnp
from jax import lax
from jax.experimental import pallas as pl
from jax.experimental.pallas import tpu as pltpu
from jax.sharding import PartitionSpec as P

STEPS = 2
modulus = 0.1
time_step = 0.5
MESH = pl.DeviceIdType.MESH

CX, RY, NZ = 6, 8, 128
PLANES, ROWS = 3 * CX + 5, 3 * RY
X0, Y0 = CX, RY
LINE = 25
OWN = slice(Y0, Y0 + RY)
F32 = jnp.float32


def bond_offsets():
    found = []
    for a in range(-3, 4):
        for b in range(-3, 4):
            for c in range(-3, 4):
                square = a * a + b * b + c * c
                if square == 0 or square > 9:
                    continue
                if a > 0 or (a == 0 and b > 0) or (a == 0 and b == 0 and c > 0):
                    found.append((a, b, c))
    return found


BONDS = bond_offsets()
NUMBER = {xi: k for k, xi in enumerate(BONDS)}
TURNS = (-2, -1, 1, 2)


def flag_of(xi):
    k = NUMBER[xi]
    return (0, 1 << k) if k < 31 else (1, 1 << (k - 31))


def bits_where(test):
    words = [0, 0]
    for xi in BONDS:
        if test(*xi):
            word, bit = flag_of(xi)
            words[word] |= bit
    return words


def disc(b):
    return [(a, c) for c in range(-3, 4) for a in range(-3, 4) if a * a + b * b + c * c <= 9]


PLACE = {abs(b): {ac: n for n, ac in enumerate(disc(b))} for b in range(4)}
PAIRS = [
    pair
    for c in range(0, 4)
    for b in range(-3, 4)
    if b * b + c * c <= 9 and (c > 0 or b >= 0)
    for pair in dict.fromkeys(((b, c), (-b, -c)))
]


def reach(b, c):
    return max(a for a in range(4) if a * a + b * b + c * c <= 9)


def strength(a, b, c):
    return time_step * (modulus / float(a * a + b * b + c * c) ** 1.5)


def combine(terms):
    terms = sorted(terms, key=lambda kv: isinstance(kv[0], (int, float)) and kv[0] < 0)
    out = None
    for k, v in terms:
        if not isinstance(k, (int, float)):
            out = v * k if out is None else out + v * k
            continue
        if k == 0:
            continue
        w = v if abs(k) == 1 else v * F32(abs(k))
        if out is None:
            out = w if k > 0 else -w
        else:
            out = out + w if k > 0 else out - w
    return out


SEND_GROUPS = (
    ("over", "over_v"),
    ("right", "over_right", "right_v", "over_right_v"),
    ("left", "over_left", "left_v", "over_left_v"),
)
RECV_GROUPS = (
    ("over",),
    ("left", "over_left"),
    ("right", "over_right"),
    ("over_v",),
    ("left_v", "over_left_v"),
    ("right_v", "over_right_v"),
)
SEND_SLOT = {name: slot for slot, names in enumerate(SEND_GROUPS) for name in names}
RECV_SLOT = {name: slot for slot, names in enumerate(RECV_GROUPS) for name in names}


def copies(side, refs, sems, bar, lat):
    u, v, flags = refs
    send, recv = sems

    def rows(ref, lead, src, dst, n):
        here = pl.ds(2 * RY - n - side * (RY - n), n)
        there = pl.ds(RY - n + side * (RY + n), n)
        return ref.at[lead, src, here], ref.at[lead, dst, there]

    def tile(ref, lead, src, dst):
        return ref.at[lead, src, OWN], ref.at[lead, dst, OWN]

    every = slice(None)
    own = slice(6, 12)
    plan = {
        "over_right": [
            rows(u, every, slice(7, 12), slice(1, 6), 5),
            rows(flags, every, slice(7, 12), slice(1, 6), 5),
        ],
        "right": [
            tile(u, every, slice(7, 12), slice(1, 6)),
            tile(flags, 1, own, slice(0, 6)),
            tile(flags, 0, slice(8, 12), slice(2, 6)),
            tile(u, 0, slice(6, 7), slice(0, 1)),
        ],
        "over_left": [
            rows(u, every, slice(6, 11), slice(12, 17), 5),
            rows(flags, every, slice(6, 9), slice(12, 15), 5),
        ],
        "left": [
            tile(u, every, slice(6, 11), slice(12, 17)),
            tile(flags, every, slice(6, 9), slice(12, 15)),
            tile(u, 0, slice(11, 12), slice(17, 18)),
        ],
        "over": [rows(u, every, own, own, 6), rows(flags, every, own, own, 6)],
        "over_right_v": [rows(v, every, slice(10, 12), slice(4, 6), 2)],
        "right_v": [tile(v, every, slice(10, 12), slice(4, 6)), tile(v, 0, slice(9, 10), slice(3, 4))],
        "over_left_v": [rows(v, every, slice(6, 8), slice(12, 14), 2)],
        "left_v": [tile(v, every, slice(6, 8), slice(12, 14)), tile(v, 0, slice(8, 9), slice(14, 15))],
        "over_v": [rows(v, every, own, own, 3)],
    }
    partner = {
        "right": (bar + 1, lat),
        "left": (bar - 1, lat),
        "over": (bar, 1 - lat),
        "over_right": (bar + 1, 1 - lat),
        "over_left": (bar - 1, 1 - lat),
    }
    made = {}
    for name, pairs in plan.items():
        made[name] = []
        where = partner[name.removesuffix("_v")]
        for src, dst in pairs:
            made[name].append(
                functools.partial(
                    pltpu.make_async_remote_copy,
                    src_ref=src,
                    dst_ref=dst,
                    send_sem=send.at[SEND_SLOT[name]],
                    recv_sem=recv.at[RECV_SLOT[name]],
                    device_id={"bar": where[0], "lat": where[1]},
                    device_id_type=MESH,
                )
            )
    return made


def kernel(
    bars,
    u_hbm, v_hbm, low_hbm, high_hbm, bc_hbm,
    base_out, half_out,
    frame, flags, vel, speeds, bc, lines, marks, turned, spun, weight, local, send, recv,
):
    bar, lat = lax.axis_index("bar"), lax.axis_index("lat")
    has_left, has_right = bar > 0, bar < bars - 1
    flat_frame = frame.reshape(STEPS, 3, PLANES * ROWS, NZ)
    flat_vel = vel.reshape(3, PLANES * ROWS, NZ)
    flat_turned = turned.reshape(STEPS, 5, 3, PLANES * ROWS, NZ)

    loads = [
        pltpu.make_async_copy(low_hbm, flags.at[0, X0:X0 + CX, OWN], local.at[0]),
        pltpu.make_async_copy(high_hbm, flags.at[1, X0:X0 + CX, OWN], local.at[1]),
        pltpu.make_async_copy(u_hbm, frame.at[0, :, X0:X0 + CX, OWN], local.at[2]),
        pltpu.make_async_copy(v_hbm, vel.at[:, X0:X0 + CX, OWN], local.at[3]),
        pltpu.make_async_copy(bc_hbm, bc, local.at[4]),
    ]
    barrier = pltpu.get_barrier_semaphore()

    def greet(b, l):
        pl.semaphore_signal(barrier, inc=1, device_id={"bar": b, "lat": l}, device_id_type=MESH)

    greet(bar, 1 - lat)

    @pl.when(has_left)
    def _():
        greet(bar - 1, lat)
        greet(bar - 1, 1 - lat)

    @pl.when(has_right)
    def _():
        greet(bar + 1, lat)
        greet(bar + 1, 1 - lat)

    for copy in loads:
        copy.start()

    void = pl.ds(pl.multiple_of(lat * (2 * RY), RY), RY)
    halo_start = pl.multiple_of((1 - lat) * (2 * RY), RY)
    halo = pl.ds(halo_start, RY)
    for step, first, last in ((0, 1, 17), (1, 4, 14)):
        zero = jnp.zeros((last - first, RY, NZ), F32)
        for comp in range(3):
            if comp < 2:
                frame[step, comp, first:last, void, :] = zero
            for c in TURNS:
                turned[step, c + 2, comp, first:last, void, :] = zero
    for word in range(2):
        flags[word, 0:15, void, :] = jnp.full((15, RY, NZ), -1, jnp.int32)
        for c in TURNS:
            spun[word, c + 2, 1:15, void, :] = jnp.full((14, RY, NZ), -1, jnp.int32)

    @pl.when(jnp.logical_not(has_left))
    def _():
        for comp in range(3):
            frame[0, comp, 0:6] = jnp.zeros((6, ROWS, NZ), F32)
            vel[comp, 3:6] = jnp.zeros((3, ROWS, NZ), F32)
        for word in range(2):
            flags[word, 0:6] = jnp.full((6, ROWS, NZ), -1, jnp.int32)

    @pl.when(jnp.logical_not(has_right))
    def _():
        for comp in range(3):
            frame[0, comp, 12:18] = jnp.zeros((6, ROWS, NZ), F32)
            vel[comp, 12:15] = jnp.zeros((3, ROWS, NZ), F32)

    sems = (send, recv)
    refs = (frame.at[0], vel, flags)
    sent = copies(lat, refs, sems, bar, lat)

    def when_there(condition, run):
        if condition is None:
            run()
        else:
            pl.when(condition)(run)

    def send_all():
        for name, made in sent.items():
            there = {"right": has_right, "left": has_left}.get(name.removesuffix("_v").split("_")[-1])

            def run():
                for copy in made:
                    copy().start()

            when_there(there, run)

    def wait_group(names, sem, there):
        lines_sent = sum(
            copy.keywords["src_ref"].shape[0] * copy.keywords["src_ref"].shape[1] * copy.keywords["src_ref"].shape[2]
            if len(copy.keywords["src_ref"].shape) == 4
            else copy.keywords["src_ref"].shape[0] * copy.keywords["src_ref"].shape[1]
            for name in names
            for copy in sent[name]
        )

        def run():
            total = lines.at[0, 0, 0:lines_sent]
            pltpu.make_async_copy(total, total, sem).wait()

        when_there(there, run)

    def received(*names):
        there = {"right": has_left, "left": has_right}.get(names[0].removesuffix("_v"))
        wait_group(names, recv.at[RECV_GROUPS.index(names)], there)

    def all_sent():
        for slot, there in enumerate((None, has_right, has_left)):
            wait_group(SEND_GROUPS[slot], send.at[slot], there)

    row = lax.broadcasted_iota(jnp.int32, (RY, NZ), 0)
    lane = lax.broadcasted_iota(jnp.int32, (RY, NZ), 1)
    for copy in loads[:2]:
        copy.wait()
    for word in range(2):
        gone = jnp.zeros((RY, NZ), jnp.int32)
        for t in range(3):
            under = bits_where(lambda a, b, c: b < -t)[word]
            above = bits_where(lambda a, b, c: b > t)[word]
            cut = jnp.where(lat == 0, jnp.int32(under), jnp.int32(above))
            gone = jnp.where(row == t + lat * (RY - 1 - 2 * t), cut, gone)
        for t in range(3):
            under = bits_where(lambda a, b, c: c < -t)[word]
            above = bits_where(lambda a, b, c: c > t)[word]
            gone = jnp.where(lane == t, gone | jnp.int32(under), gone)
            gone = jnp.where(lane == NZ - 1 - t, gone | jnp.int32(above), gone)
        for x in range(CX):
            flags[word, X0 + x, OWN, :] = flags[word, X0 + x, OWN, :] | gone

    @pl.when(jnp.logical_not(has_right))
    def _():
        for x in range(3, CX):
            beyond = bits_where(lambda a, b, c: x + a >= CX)
            for word in range(2):
                flags[word, X0 + x, OWN, :] = flags[word, X0 + x, OWN, :] | jnp.int32(beyond[word])

    for copy in loads[2:]:
        copy.wait()
    sign = 1 - 2 * lat
    fsign = sign.astype(F32)
    edge_row = {d: Y0 + RY - 1 + d - lat * (RY - 1 + 2 * d) for d in (1, 2, 3)}

    class Tile:
        def __init__(self, plane):
            self.plane = plane

        def get(self, ref, lead, a, b):
            return ref[(*lead, X0 + self.plane + a, pl.ds(Y0 + b, RY), slice(None))]

        def put(self, ref, flat, lead, value):
            ref[(*lead, X0 + self.plane, OWN, slice(None))] = value

    class Row:
        def __init__(self, plane, d):
            self.plane, self.d = plane, d

        def get(self, ref, lead, a, b):
            at = pl.ds(edge_row[self.d] * LINE + ((X0 + self.plane + a) + b * LINE), RY)
            if ref is frame:
                return lines[2, lead[1], at, :]
            if ref is turned:
                return lines[lead[1], lead[2], at, :]
            if ref is flags:
                return marks[lead[0], 2, at, :]
            if ref is spun:
                return marks[lead[0], lead[1], at, :]
            return flat_vel[(*lead, self.strided(), slice(None))]

        def strided(self):
            return pl.ds(edge_row[self.d] + (X0 + self.plane) * ROWS, RY, stride=ROWS)

        def put(self, ref, flat, lead, value):
            flat[(*lead, self.strided(), slice(None))] = value

    def line(plane, rows):
        return pl.ds((Y0 * LINE if rows is OWN else halo_start * LINE) + plane, RY, stride=LINE)

    def spin(plane, rows, turns=(-2, -1, 0, 1, 2)):
        for word in range(2):
            held = flags[word, plane, rows, :]
            for c in turns:
                moved = pltpu.roll(held, (-c) % NZ, axis=1) if c else held
                marks[word, c + 2, line(plane, rows), :] = moved
                if c:
                    spun[word, c + 2, plane, rows, :] = moved

    def turn(plane, rows, turns=(-2, -1, 0, 1, 2)):
        for comp in range(3):
            held = frame[0, comp, plane, rows, :]
            for c in turns:
                moved = combine([(c if comp == 2 else 1, pltpu.roll(held, (-c) % NZ, axis=1))]) if c else held
                lines[c + 2, comp, line(plane, rows), :] = moved
                if c:
                    turned[0, c + 2, comp, plane, rows, :] = moved

    def put_weight(xi, back, planes):
        a, b, c = xi
        word, bit = flag_of(xi)
        a1, b1, c1 = (-a, -b, -c) if back else xi
        place = PLACE[abs(b1)][(a1, c1)]
        for x in planes:
            if not back:
                held = flags[word, X0 + x, OWN, :]
            elif c == 0:
                held = flags[word, X0 + x + a1, Y0 + b1:Y0 + b1 + RY, :]
            elif c == 3:
                held = pltpu.roll(flags[word, X0 + x, OWN, :], 3, axis=1)
            else:
                held = spun[word, c1 + 2, X0 + x + a1, Y0 + b1:Y0 + b1 + RY, :]
            weight[b1 + 3, place, x] = jnp.where((held & jnp.int32(bit)) == 0, F32(strength(*xi)), F32(0.0))

    heres = {}

    def add_terms(step, b, shift, factor, c, tasks):
        seen = {}
        opposite = (step, -b, -c)
        for key in list(heres):
            if key[:3] != opposite:
                del heres[key]
        for group, todo, force, want, table in tasks:
            if 0 not in want:
                todo = todo if (b or c) and (1 not in want or b or 2 in want) else []
            elif want == (0,):
                todo = [a for a in todo if a]
            todo = [a for a in todo if a or b or c]
            if not todo:
                continue

            def fetch(comp, a):
                if c == 0:
                    return group.get(frame, (step, comp), a, shift)
                return group.get(turned, (step, c + 2, comp), a, shift)

            def mine(comp):
                return group.get(frame, (step, comp), 0, 0)

            def nearby(a):
                key = (group.plane + a, isinstance(group, Row) and group.d)
                if key not in seen:
                    terms = []
                    if abs(c) == 3:
                        terms.append((c, pltpu.roll(mine(2), (-c) % NZ, axis=1)))
                    elif c:
                        terms.append((1, fetch(2, a)))
                    if b:
                        terms.append((factor, fetch(1, a)))
                    seen[key] = combine(terms)
                return seen[key]

            def kept(a, value):
                if table is not None:
                    return table[PLACE[abs(b)][(a, c)], group.plane] * value
                if (a, b, c) in NUMBER:
                    word, bit = flag_of((a, b, c))
                    held = group.get(flags, (word,), 0, 0)
                else:
                    word, bit = flag_of((-a, -b, -c))
                    if c == 0:
                        held = group.get(flags, (word,), a, b)
                    elif c == -3:
                        held = pltpu.roll(group.get(flags, (word,), 0, 0), 3, axis=1)
                    else:
                        held = group.get(spun, (word, c + 2), a, b)
                return jnp.where((held & jnp.int32(bit)) == 0, value, F32(0.0))

            needs = [a for a in todo if (*opposite, -a, group) not in heres]
            mine0 = mine(0) if any(needs) else None
            alone = not b and not c
            base = combine([(factor, mine(1))] * bool(b) + [(c, mine(2))] * bool(c)) if needs else None
            pulls = {}
            for a in todo:
                if alone:
                    pulls[a] = kept(a, fetch(0, a) - mine0)
                    continue
                there = nearby(a)
                if a:
                    there = combine([(1, there), (a, fetch(0, a))])
                if a in needs:
                    here = combine([(1, base), (a, mine0)]) if a else base
                    heres[(step, b, c, a, group)] = here
                    pulls[a] = kept(a, there - here)
                else:
                    pulls[a] = kept(a, there + heres[(*opposite, -a, group)])
            total, along = None, None
            for size in range(4):
                plus, minus = pulls.get(size), pulls.get(-size) if size else None
                if plus is None and minus is None:
                    continue
                k = 1.0 if table is not None else strength(size, b, c)
                if alone:
                    both = combine([(1, v) for v in (plus, minus) if v is not None])
                    along = combine([(1, along)] * (along is not None) + [(k * size * size, both)])
                    continue
                both = combine([(1, v) for v in (plus, minus) if v is not None])
                total = combine([(1, total)] * (total is not None) + [(k, both)])
                if size and 0 in want:
                    if plus is None:
                        term = (-k * size, minus)
                    elif minus is None:
                        term = (k * size, plus)
                    else:
                        term = (k * size, plus - minus)
                    along = combine([(1, along)] * (along is not None) + [term])
            for comp, k, value in ((0, 1, along), (1, factor, total), (2, c, total)):
                if comp not in want or value is None or (comp == 1 and not b) or (comp == 2 and not c):
                    continue
                force[comp] = combine([(1, force[comp])] * (force[comp] is not None) + [(k, value)])

    retain = {}
    for key, where in (("left", jnp.maximum(bar - 1, 0)), ("own", bar), ("right", jnp.minimum(bar + 1, bars - 1))):
        retain[key] = 1.0 - 0.2 * bc[where].astype(F32)

    def retain_of(group):
        if isinstance(group, Tile):
            return retain["left" if group.plane < 0 else "own" if group.plane < CX else "right"]
        plane = row + group.plane
        return jnp.where(plane < 0, retain["left"], jnp.where(plane < CX, retain["own"], retain["right"]))

    def advance(group, force, want=(0, 1, 2)):
        keep = retain_of(group)
        for comp in want:
            speed = keep * (group.get(vel, (comp,), 0, 0) + force[comp])
            moved = group.get(frame, (0, comp), 0, 0) + F32(time_step) * speed
            if isinstance(group, Tile) and 0 <= group.plane < CX:
                speeds[comp, group.plane] = speed
            group.put(frame, flat_frame, (1, comp), moved)
            far = (group.plane in (-3, 8)) if isinstance(group, Tile) else group.d == 3
            if not far:
                for c in TURNS:
                    value = pltpu.roll(moved, (-c) % NZ, axis=1)
                    group.put(turned, flat_turned, (1, c + 2, comp), combine([(c if comp == 2 else 1, value)]))

    def blank():
        return [None, None, None]

    def span(b, c):
        far = reach(b, c)
        return range(-far, far + 1)

    own = [Tile(x) for x in range(CX)]
    force = [blank() for _ in range(CX)]
    every = (0, 1, 2)

    def own_terms(step, beta, c, chosen, pulls):
        shift, factor = (sign * beta, fsign * F32(beta)) if beta else (0, 0)
        table = weight.at[3 + shift]
        tasks = [
            (own[x], [a for a in span(beta, c) if chosen(x, x + a)], pulls[x], every, table) for x in range(CX)
        ]
        add_terms(step, beta, shift, factor, c, tasks)

    def outer(groups_wants, chosen=lambda group, a: True):
        made = [(entry[0], entry[2] if len(entry) > 2 else blank(), entry[1]) for entry in groups_wants]
        for b, c in PAIRS:
            add_terms(
                0, b, b, b, c,
                [(group, [a for a in span(b, c) if chosen(group, a)], pull, want, None) for group, pull, want in made],
            )
        return made

    def advance_all(made):
        for group, pull, want in made:
            advance(group, pull, want)

    pl.semaphore_wait(barrier, 1 + 2 * has_left.astype(jnp.int32) + 2 * has_right.astype(jnp.int32))
    send_all()

    for x in range(CX):
        spin(X0 + x, OWN)
        turn(X0 + x, OWN)
    for xi in BONDS:
        put_weight(xi, False, range(CX))
    for xi in BONDS:
        if xi[1] == 0:
            put_weight(xi, True, range(xi[0], CX))
    for side in range(2):

        @pl.when(lat == side)
        def _():
            for xi in BONDS:
                if xi[1] * (1 - 2 * side) > 0:
                    put_weight(xi, True, range(xi[0], CX))

    for beta, c in PAIRS:
        if beta <= 0:
            own_terms(0, beta, c, lambda x, q: 0 <= q < CX, force)

    received("left", "over_left")
    for plane in range(12, 17):
        turn(plane, OWN)
        turn(plane, halo)
    for plane in range(12, 15):
        spin(plane, OWN)
        spin(plane, halo)
    for b, c in PAIRS:
        add_terms(0, b, b, b, c, [
            (own[x], [a for a in span(b, c) if x + a >= CX], force[x], every, weight.at[3 + b]) for x in range(CX)
        ])
    right_tiles = [(Tile(6), every, blank()), (Tile(7), every, blank()), (Tile(8), (0,), blank())]
    right_rows = [(Row(6, d), every, blank()) for d in (1, 2)]
    outer(right_tiles, lambda group, a: group.plane + a >= CX)
    for entry in right_rows:
        outer([entry], lambda group, a: a >= 0)

    received("over")
    for x in range(CX):
        spin(X0 + x, halo)
        turn(X0 + x, halo)
    for side in range(2):

        @pl.when(lat == side)
        def _():
            for xi in BONDS:
                if xi[1] * (1 - 2 * side) < 0:
                    put_weight(xi, True, range(xi[0], CX))

    for beta, c in PAIRS:
        if beta > 0:
            own_terms(0, beta, c, lambda x, q: 0 <= q < CX, force)
    for x in range(3, CX):
        advance(own[x], force[x])
    made = outer(right_tiles, lambda group, a: group.plane + a < CX)
    received("left_v", "over_left_v")
    advance_all(made)
    made = []
    for entry in right_rows:
        made += outer([entry], lambda group, a: a < 0)
    received("over_v")
    advance_all(made)
    third = blank()
    outer([(Row(0, 3), (1,), third)], lambda group, a: a >= 0)
    again = [blank() for _ in range(CX)]

    def early(x, q):
        return x >= 3 and q >= 3

    for beta, c in PAIRS:
        if beta <= 0:
            own_terms(1, beta, c, early, again)

    all_sent()
    received("right", "over_right")
    for plane in range(1, 6):
        spin(plane, OWN)
        turn(plane, OWN)
        spin(plane, halo)
        turn(plane, halo)
    for xi in BONDS:
        put_weight(xi, True, range(min(xi[0], CX)))
    for beta, c in PAIRS:
        own_terms(0, beta, c, lambda x, q: q < 0, force)
    for x in range(3):
        advance(own[x], force[x])
    made = outer([(Tile(-3), (0,)), (Tile(-2), every), (Tile(-1), every)])
    received("right_v", "over_right_v")
    advance_all(made)
    made = outer([(Row(-2, 1), every)]) + outer([(Row(-2, 2), every)])
    made += outer([(Row(0, 3), (1,), third)], lambda group, a: a < 0)
    advance_all(made)

    for beta, c in PAIRS:
        own_terms(1, beta, c, (lambda x, q: not early(x, q)) if beta <= 0 else (lambda x, q: True), again)
    for x in range(CX):
        for comp in range(3):
            speed = retain["own"] * (speeds[comp, x] + again[x][comp])
            half_out[comp, x] = F32(time_step) * speed
            base_out[comp, x] = frame[1, comp, X0 + x, OWN, :]


def local_steps(bars, displace, velocity, bond_low, bond_high, bc_type):
    any_space = pl.BlockSpec(memory_space=pl.ANY)
    out = pltpu.VMEM(displace.shape, F32)
    base, half = pl.pallas_call(
        functools.partial(kernel, bars),
        out_shape=(out, out),
        in_specs=[any_space] * 5,
        scratch_shapes=[
            pltpu.VMEM((STEPS, 3, PLANES, ROWS, NZ), F32),
            pltpu.VMEM((2, PLANES, ROWS, NZ), jnp.int32),
            pltpu.VMEM((3, PLANES, ROWS, NZ), F32),
            pltpu.VMEM((3, CX, RY, NZ), F32),
            pltpu.SMEM((bc_type.shape[0],), jnp.int32),
            pltpu.VMEM((5, 3, ROWS * LINE, NZ), F32),
            pltpu.VMEM((2, 5, ROWS * LINE, NZ), jnp.int32),
            pltpu.VMEM((STEPS, 5, 3, PLANES, ROWS, NZ), F32),
            pltpu.VMEM((2, 5, PLANES, ROWS, NZ), jnp.int32),
            pltpu.VMEM((7, 29, CX, RY, NZ), F32),
            pltpu.SemaphoreType.DMA((5,)),
            pltpu.SemaphoreType.DMA((len(SEND_GROUPS),)),
            pltpu.SemaphoreType.DMA((len(RECV_GROUPS),)),
        ],
        compiler_params=pltpu.CompilerParams(collective_id=0, has_side_effects=True),
        name="peridynamics",
    )(displace, velocity, bond_low, bond_high, bc_type)
    return base + half, half + half


def solution(mesh):
    bars = mesh.shape["bar"]
    return jax.shard_map(
        functools.partial(local_steps, bars),
        mesh=mesh,
        in_specs=(
            P(None, "bar", "lat", None),
            P(None, "bar", "lat", None),
            P("bar", "lat", None),
            P("bar", "lat", None),
            P(),
        ),
        out_specs=(P(None, "bar", "lat", None), P(None, "bar", "lat", None)),
        check_vma=False,
    )
```

```python
import functools

import jax
import jax.numpy as jnp
from jax import lax
from jax.experimental import pallas as pl
from jax.experimental.pallas import tpu as pltpu
from jax.sharding import PartitionSpec as P

STEPS = 2
modulus = 0.1
time_step = 0.5
MESH = pl.DeviceIdType.MESH

CX, RY, NZ = 6, 8, 128
PLANES, ROWS = 3 * CX + 5, 3 * RY
X0, Y0 = CX, RY
LINE = 25
OWN = slice(Y0, Y0 + RY)
F32 = jnp.float32


def bond_offsets():
    found = []
    for a in range(-3, 4):
        for b in range(-3, 4):
            for c in range(-3, 4):
                square = a * a + b * b + c * c
                if square == 0 or square > 9:
                    continue
                if a > 0 or (a == 0 and b > 0) or (a == 0 and b == 0 and c > 0):
                    found.append((a, b, c))
    return found


BONDS = bond_offsets()
NUMBER = {xi: k for k, xi in enumerate(BONDS)}
TURNS = (-2, -1, 1, 2)


def flag_of(xi):
    k = NUMBER[xi]
    return (0, 1 << k) if k < 31 else (1, 1 << (k - 31))


def bits_where(test):
    words = [0, 0]
    for xi in BONDS:
        if test(*xi):
            word, bit = flag_of(xi)
            words[word] |= bit
    return words


def disc(b):
    return [(a, c) for c in range(-3, 4) for a in range(-3, 4) if a * a + b * b + c * c <= 9]


PLACE = {abs(b): {ac: n for n, ac in enumerate(disc(b))} for b in range(4)}
PAIRS = [
    pair
    for c in range(0, 4)
    for b in range(-3, 4)
    if b * b + c * c <= 9 and (c > 0 or b >= 0)
    for pair in dict.fromkeys(((b, c), (-b, -c)))
]


def reach(b, c):
    return max(a for a in range(4) if a * a + b * b + c * c <= 9)


def strength(a, b, c):
    return time_step * (modulus / float(a * a + b * b + c * c) ** 1.5)


def combine(terms):
    terms = sorted(terms, key=lambda kv: isinstance(kv[0], (int, float)) and kv[0] < 0)
    out = None
    for k, v in terms:
        if not isinstance(k, (int, float)):
            out = v * k if out is None else out + v * k
            continue
        if k == 0:
            continue
        w = v if abs(k) == 1 else v * F32(abs(k))
        if out is None:
            out = w if k > 0 else -w
        else:
            out = out + w if k > 0 else out - w
    return out


SEND_GROUPS = (
    ("over", "over_v"),
    ("right", "over_right", "right_v", "over_right_v"),
    ("left", "over_left", "left_v", "over_left_v"),
)
RECV_GROUPS = (
    ("over",),
    ("left", "over_left"),
    ("right", "over_right"),
    ("over_v",),
    ("left_v", "over_left_v"),
    ("right_v", "over_right_v"),
)
SEND_SLOT = {name: slot for slot, names in enumerate(SEND_GROUPS) for name in names}
RECV_SLOT = {name: slot for slot, names in enumerate(RECV_GROUPS) for name in names}


def copies(side, refs, sems, bar, lat):
    u, v, flags = refs
    send, recv = sems

    def rows(ref, lead, src, dst, n):
        here = pl.ds(2 * RY - n - side * (RY - n), n)
        there = pl.ds(RY - n + side * (RY + n), n)
        return ref.at[lead, src, here], ref.at[lead, dst, there]

    def tile(ref, lead, src, dst):
        return ref.at[lead, src, OWN], ref.at[lead, dst, OWN]

    every = slice(None)
    own = slice(6, 12)
    plan = {
        "over_right": [
            rows(u, every, slice(7, 12), slice(1, 6), 5),
            rows(flags, every, slice(7, 12), slice(1, 6), 5),
        ],
        "right": [
            tile(u, every, slice(7, 12), slice(1, 6)),
            tile(flags, 1, own, slice(0, 6)),
            tile(flags, 0, slice(8, 12), slice(2, 6)),
            tile(u, 0, slice(6, 7), slice(0, 1)),
        ],
        "over_left": [
            rows(u, every, slice(6, 11), slice(12, 17), 5),
            rows(flags, every, slice(6, 9), slice(12, 15), 5),
        ],
        "left": [
            tile(u, every, slice(6, 11), slice(12, 17)),
            tile(flags, every, slice(6, 9), slice(12, 15)),
            tile(u, 0, slice(11, 12), slice(17, 18)),
        ],
        "over": [rows(u, every, own, own, 6), rows(flags, every, own, own, 6)],
        "over_right_v": [rows(v, every, slice(10, 12), slice(4, 6), 2)],
        "right_v": [tile(v, every, slice(10, 12), slice(4, 6)), tile(v, 0, slice(9, 10), slice(3, 4))],
        "over_left_v": [rows(v, every, slice(6, 8), slice(12, 14), 2)],
        "left_v": [tile(v, every, slice(6, 8), slice(12, 14)), tile(v, 0, slice(8, 9), slice(14, 15))],
        "over_v": [rows(v, every, own, own, 3)],
    }
    partner = {
        "right": (bar + 1, lat),
        "left": (bar - 1, lat),
        "over": (bar, 1 - lat),
        "over_right": (bar + 1, 1 - lat),
        "over_left": (bar - 1, 1 - lat),
    }
    made = {}
    for name, pairs in plan.items():
        made[name] = []
        where = partner[name.removesuffix("_v")]
        for src, dst in pairs:
            made[name].append(
                functools.partial(
                    pltpu.make_async_remote_copy,
                    src_ref=src,
                    dst_ref=dst,
                    send_sem=send.at[SEND_SLOT[name]],
                    recv_sem=recv.at[RECV_SLOT[name]],
                    device_id={"bar": where[0], "lat": where[1]},
                    device_id_type=MESH,
                )
            )
    return made


def kernel(
    bars,
    u_hbm, v_hbm, low_hbm, high_hbm, bc_hbm,
    base_out, half_out,
    frame, flags, vel, speeds, bc, lines, marks, turned, spun, weight, local, send, recv,
):
    bar, lat = lax.axis_index("bar"), lax.axis_index("lat")
    has_left, has_right = bar > 0, bar < bars - 1
    flat_frame = frame.reshape(STEPS, 3, PLANES * ROWS, NZ)
    flat_vel = vel.reshape(3, PLANES * ROWS, NZ)
    flat_turned = turned.reshape(STEPS, 5, 3, PLANES * ROWS, NZ)

    loads = [
        pltpu.make_async_copy(low_hbm, flags.at[0, X0:X0 + CX, OWN], local.at[0]),
        pltpu.make_async_copy(high_hbm, flags.at[1, X0:X0 + CX, OWN], local.at[1]),
        pltpu.make_async_copy(u_hbm, frame.at[0, :, X0:X0 + CX, OWN], local.at[2]),
        pltpu.make_async_copy(v_hbm, vel.at[:, X0:X0 + CX, OWN], local.at[3]),
        pltpu.make_async_copy(bc_hbm, bc, local.at[4]),
    ]
    barrier = pltpu.get_barrier_semaphore()

    def greet(b, l):
        pl.semaphore_signal(barrier, inc=1, device_id={"bar": b, "lat": l}, device_id_type=MESH)

    greet(bar, 1 - lat)

    @pl.when(has_left)
    def _():
        greet(bar - 1, lat)
        greet(bar - 1, 1 - lat)

    @pl.when(has_right)
    def _():
        greet(bar + 1, lat)
        greet(bar + 1, 1 - lat)

    for copy in loads:
        copy.start()

    void = pl.ds(pl.multiple_of(lat * (2 * RY), RY), RY)
    halo_start = pl.multiple_of((1 - lat) * (2 * RY), RY)
    halo = pl.ds(halo_start, RY)
    for step, first, last in ((0, 1, 17), (1, 4, 14)):
        zero = jnp.zeros((last - first, RY, NZ), F32)
        for comp in range(3):
            if comp < 2:
                frame[step, comp, first:last, void, :] = zero
            for c in TURNS:
                turned[step, c + 2, comp, first:last, void, :] = zero
    for word in range(2):
        flags[word, 0:15, void, :] = jnp.full((15, RY, NZ), -1, jnp.int32)
        for c in TURNS:
            spun[word, c + 2, 1:15, void, :] = jnp.full((14, RY, NZ), -1, jnp.int32)

    @pl.when(jnp.logical_not(has_left))
    def _():
        for comp in range(3):
            frame[0, comp, 0:6] = jnp.zeros((6, ROWS, NZ), F32)
            vel[comp, 3:6] = jnp.zeros((3, ROWS, NZ), F32)
        for word in range(2):
            flags[word, 0:6] = jnp.full((6, ROWS, NZ), -1, jnp.int32)

    @pl.when(jnp.logical_not(has_right))
    def _():
        for comp in range(3):
            frame[0, comp, 12:18] = jnp.zeros((6, ROWS, NZ), F32)
            vel[comp, 12:15] = jnp.zeros((3, ROWS, NZ), F32)

    sems = (send, recv)
    refs = (frame.at[0], vel, flags)
    sent = copies(lat, refs, sems, bar, lat)

    def when_there(condition, run):
        if condition is None:
            run()
        else:
            pl.when(condition)(run)

    def send_all():
        even = lax.rem(bar, 2) == 0
        odd = jnp.logical_not(even)
        order = (
            ('over', even),
            ('over_v', even),
            ('over_right', None),
            ('right', None),
            ('right_v', None),
            ('over_right_v', None),
            ('over', odd),
            ('over_left', None),
            ('left', None),
            ('over_v', odd),
            ('over_left_v', None),
            ('left_v', None),
        )
        for name, there in order:
            made = sent[name]
            if there is None:
                there = {"right": has_right, "left": has_left}.get(name.removesuffix("_v").split("_")[-1])

            def run():
                for copy in made:
                    copy().start()

            when_there(there, run)

    def wait_group(names, sem, there):
        lines_sent = sum(
            copy.keywords["src_ref"].shape[0] * copy.keywords["src_ref"].shape[1] * copy.keywords["src_ref"].shape[2]
            if len(copy.keywords["src_ref"].shape) == 4
            else copy.keywords["src_ref"].shape[0] * copy.keywords["src_ref"].shape[1]
            for name in names
            for copy in sent[name]
        )

        def run():
            total = lines.at[0, 0, 0:lines_sent]
            pltpu.make_async_copy(total, total, sem).wait()

        when_there(there, run)

    def received(*names):
        there = {"right": has_left, "left": has_right}.get(names[0].removesuffix("_v"))
        wait_group(names, recv.at[RECV_GROUPS.index(names)], there)

    def all_sent():
        for slot, there in enumerate((None, has_right, has_left)):
            wait_group(SEND_GROUPS[slot], send.at[slot], there)

    row = lax.broadcasted_iota(jnp.int32, (RY, NZ), 0)
    lane = lax.broadcasted_iota(jnp.int32, (RY, NZ), 1)
    for copy in loads[:2]:
        copy.wait()
    for word in range(2):
        gone = jnp.zeros((RY, NZ), jnp.int32)
        for t in range(3):
            under = bits_where(lambda a, b, c: b < -t)[word]
            above = bits_where(lambda a, b, c: b > t)[word]
            cut = jnp.where(lat == 0, jnp.int32(under), jnp.int32(above))
            gone = jnp.where(row == t + lat * (RY - 1 - 2 * t), cut, gone)
        for t in range(3):
            under = bits_where(lambda a, b, c: c < -t)[word]
            above = bits_where(lambda a, b, c: c > t)[word]
            gone = jnp.where(lane == t, gone | jnp.int32(under), gone)
            gone = jnp.where(lane == NZ - 1 - t, gone | jnp.int32(above), gone)
        for x in range(CX):
            flags[word, X0 + x, OWN, :] = flags[word, X0 + x, OWN, :] | gone

    @pl.when(jnp.logical_not(has_right))
    def _():
        for x in range(3, CX):
            beyond = bits_where(lambda a, b, c: x + a >= CX)
            for word in range(2):
                flags[word, X0 + x, OWN, :] = flags[word, X0 + x, OWN, :] | jnp.int32(beyond[word])

    for copy in loads[2:]:
        copy.wait()
    sign = 1 - 2 * lat
    fsign = sign.astype(F32)
    edge_row = {d: Y0 + RY - 1 + d - lat * (RY - 1 + 2 * d) for d in (1, 2, 3)}

    class Tile:
        def __init__(self, plane):
            self.plane = plane

        def get(self, ref, lead, a, b):
            return ref[(*lead, X0 + self.plane + a, pl.ds(Y0 + b, RY), slice(None))]

        def put(self, ref, flat, lead, value):
            ref[(*lead, X0 + self.plane, OWN, slice(None))] = value

    class Row:
        def __init__(self, plane, d):
            self.plane, self.d = plane, d

        def get(self, ref, lead, a, b):
            at = pl.ds(edge_row[self.d] * LINE + ((X0 + self.plane + a) + b * LINE), RY)
            if ref is frame:
                return lines[2, lead[1], at, :]
            if ref is turned:
                return lines[lead[1], lead[2], at, :]
            if ref is flags:
                return marks[lead[0], 2, at, :]
            if ref is spun:
                return marks[lead[0], lead[1], at, :]
            return flat_vel[(*lead, self.strided(), slice(None))]

        def strided(self):
            return pl.ds(edge_row[self.d] + (X0 + self.plane) * ROWS, RY, stride=ROWS)

        def put(self, ref, flat, lead, value):
            flat[(*lead, self.strided(), slice(None))] = value

    def line(plane, rows):
        return pl.ds((Y0 * LINE if rows is OWN else halo_start * LINE) + plane, RY, stride=LINE)

    def spin(plane, rows, turns=(-2, -1, 0, 1, 2)):
        for word in range(2):
            held = flags[word, plane, rows, :]
            for c in turns:
                moved = pltpu.roll(held, (-c) % NZ, axis=1) if c else held
                marks[word, c + 2, line(plane, rows), :] = moved
                if c:
                    spun[word, c + 2, plane, rows, :] = moved

    def turn(plane, rows, turns=(-2, -1, 0, 1, 2)):
        for comp in range(3):
            held = frame[0, comp, plane, rows, :]
            for c in turns:
                moved = combine([(c if comp == 2 else 1, pltpu.roll(held, (-c) % NZ, axis=1))]) if c else held
                lines[c + 2, comp, line(plane, rows), :] = moved
                if c:
                    turned[0, c + 2, comp, plane, rows, :] = moved

    def put_weight(xi, back, planes):
        a, b, c = xi
        word, bit = flag_of(xi)
        a1, b1, c1 = (-a, -b, -c) if back else xi
        place = PLACE[abs(b1)][(a1, c1)]
        for x in planes:
            if not back:
                held = flags[word, X0 + x, OWN, :]
            elif c == 0:
                held = flags[word, X0 + x + a1, Y0 + b1:Y0 + b1 + RY, :]
            elif c == 3:
                held = pltpu.roll(flags[word, X0 + x, OWN, :], 3, axis=1)
            else:
                held = spun[word, c1 + 2, X0 + x + a1, Y0 + b1:Y0 + b1 + RY, :]
            weight[b1 + 3, place, x] = jnp.where((held & jnp.int32(bit)) == 0, F32(strength(*xi)), F32(0.0))

    heres = {}

    def add_terms(step, b, shift, factor, c, tasks):
        seen = {}
        opposite = (step, -b, -c)
        for key in list(heres):
            if key[:3] != opposite:
                del heres[key]
        for group, todo, force, want, table in tasks:
            if 0 not in want:
                todo = todo if (b or c) and (1 not in want or b or 2 in want) else []
            elif want == (0,):
                todo = [a for a in todo if a]
            todo = [a for a in todo if a or b or c]
            if not todo:
                continue

            def fetch(comp, a):
                if c == 0:
                    return group.get(frame, (step, comp), a, shift)
                return group.get(turned, (step, c + 2, comp), a, shift)

            def mine(comp):
                return group.get(frame, (step, comp), 0, 0)

            def nearby(a):
                key = (group.plane + a, isinstance(group, Row) and group.d)
                if key not in seen:
                    terms = []
                    if abs(c) == 3:
                        terms.append((c, pltpu.roll(mine(2), (-c) % NZ, axis=1)))
                    elif c:
                        terms.append((1, fetch(2, a)))
                    if b:
                        terms.append((factor, fetch(1, a)))
                    seen[key] = combine(terms)
                return seen[key]

            def kept(a, value):
                if table is not None:
                    return table[PLACE[abs(b)][(a, c)], group.plane] * value
                if (a, b, c) in NUMBER:
                    word, bit = flag_of((a, b, c))
                    held = group.get(flags, (word,), 0, 0)
                else:
                    word, bit = flag_of((-a, -b, -c))
                    if c == 0:
                        held = group.get(flags, (word,), a, b)
                    elif c == -3:
                        held = pltpu.roll(group.get(flags, (word,), 0, 0), 3, axis=1)
                    else:
                        held = group.get(spun, (word, c + 2), a, b)
                return jnp.where((held & jnp.int32(bit)) == 0, value, F32(0.0))

            needs = [a for a in todo if (*opposite, -a, group) not in heres]
            mine0 = mine(0) if any(needs) else None
            alone = not b and not c
            base = combine([(factor, mine(1))] * bool(b) + [(c, mine(2))] * bool(c)) if needs else None
            pulls = {}
            for a in todo:
                if alone:
                    pulls[a] = kept(a, fetch(0, a) - mine0)
                    continue
                there = nearby(a)
                if a:
                    there = combine([(1, there), (a, fetch(0, a))])
                if a in needs:
                    here = combine([(1, base), (a, mine0)]) if a else base
                    heres[(step, b, c, a, group)] = here
                    pulls[a] = kept(a, there - here)
                else:
                    pulls[a] = kept(a, there + heres[(*opposite, -a, group)])
            total, along = None, None
            for size in range(4):
                plus, minus = pulls.get(size), pulls.get(-size) if size else None
                if plus is None and minus is None:
                    continue
                k = 1.0 if table is not None else strength(size, b, c)
                if alone:
                    both = combine([(1, v) for v in (plus, minus) if v is not None])
                    along = combine([(1, along)] * (along is not None) + [(k * size * size, both)])
                    continue
                both = combine([(1, v) for v in (plus, minus) if v is not None])
                total = combine([(1, total)] * (total is not None) + [(k, both)])
                if size and 0 in want:
                    if plus is None:
                        term = (-k * size, minus)
                    elif minus is None:
                        term = (k * size, plus)
                    else:
                        term = (k * size, plus - minus)
                    along = combine([(1, along)] * (along is not None) + [term])
            for comp, k, value in ((0, 1, along), (1, factor, total), (2, c, total)):
                if comp not in want or value is None or (comp == 1 and not b) or (comp == 2 and not c):
                    continue
                force[comp] = combine([(1, force[comp])] * (force[comp] is not None) + [(k, value)])

    retain = {}
    for key, where in (("left", jnp.maximum(bar - 1, 0)), ("own", bar), ("right", jnp.minimum(bar + 1, bars - 1))):
        retain[key] = 1.0 - 0.2 * bc[where].astype(F32)

    def retain_of(group):
        if isinstance(group, Tile):
            return retain["left" if group.plane < 0 else "own" if group.plane < CX else "right"]
        plane = row + group.plane
        return jnp.where(plane < 0, retain["left"], jnp.where(plane < CX, retain["own"], retain["right"]))

    def advance(group, force, want=(0, 1, 2)):
        keep = retain_of(group)
        for comp in want:
            speed = keep * (group.get(vel, (comp,), 0, 0) + force[comp])
            moved = group.get(frame, (0, comp), 0, 0) + F32(time_step) * speed
            if isinstance(group, Tile) and 0 <= group.plane < CX:
                speeds[comp, group.plane] = speed
            group.put(frame, flat_frame, (1, comp), moved)
            far = (group.plane in (-3, 8)) if isinstance(group, Tile) else group.d == 3
            if not far:
                for c in TURNS:
                    value = pltpu.roll(moved, (-c) % NZ, axis=1)
                    group.put(turned, flat_turned, (1, c + 2, comp), combine([(c if comp == 2 else 1, value)]))

    def blank():
        return [None, None, None]

    def span(b, c):
        far = reach(b, c)
        return range(-far, far + 1)

    own = [Tile(x) for x in range(CX)]
    force = [blank() for _ in range(CX)]
    every = (0, 1, 2)

    def own_terms(step, beta, c, chosen, pulls):
        shift, factor = (sign * beta, fsign * F32(beta)) if beta else (0, 0)
        table = weight.at[3 + shift]
        tasks = [
            (own[x], [a for a in span(beta, c) if chosen(x, x + a)], pulls[x], every, table) for x in range(CX)
        ]
        add_terms(step, beta, shift, factor, c, tasks)

    def outer(groups_wants, chosen=lambda group, a: True):
        made = [(entry[0], entry[2] if len(entry) > 2 else blank(), entry[1]) for entry in groups_wants]
        for b, c in PAIRS:
            add_terms(
                0, b, b, b, c,
                [(group, [a for a in span(b, c) if chosen(group, a)], pull, want, None) for group, pull, want in made],
            )
        return made

    def advance_all(made):
        for group, pull, want in made:
            advance(group, pull, want)

    pl.semaphore_wait(barrier, 1 + 2 * has_left.astype(jnp.int32) + 2 * has_right.astype(jnp.int32))
    send_all()

    for x in range(CX):
        spin(X0 + x, OWN)
        turn(X0 + x, OWN)
    for xi in BONDS:
        put_weight(xi, False, range(CX))
    for xi in BONDS:
        if xi[1] == 0:
            put_weight(xi, True, range(xi[0], CX))
    for side in range(2):

        @pl.when(lat == side)
        def _():
            for xi in BONDS:
                if xi[1] * (1 - 2 * side) > 0:
                    put_weight(xi, True, range(xi[0], CX))

    for beta, c in PAIRS:
        if beta <= 0:
            own_terms(0, beta, c, lambda x, q: 0 <= q < CX, force)

    received("left", "over_left")
    for plane in range(12, 17):
        turn(plane, OWN)
        turn(plane, halo)
    for plane in range(12, 15):
        spin(plane, OWN)
        spin(plane, halo)
    for b, c in PAIRS:
        add_terms(0, b, b, b, c, [
            (own[x], [a for a in span(b, c) if x + a >= CX], force[x], every, weight.at[3 + b]) for x in range(CX)
        ])
    right_tiles = [(Tile(6), every, blank()), (Tile(7), every, blank()), (Tile(8), (0,), blank())]
    right_rows = [(Row(6, d), every, blank()) for d in (1, 2)]
    outer(right_tiles, lambda group, a: group.plane + a >= CX)
    for entry in right_rows:
        outer([entry], lambda group, a: a >= 0)

    received("over")
    for x in range(CX):
        spin(X0 + x, halo)
        turn(X0 + x, halo)
    for side in range(2):

        @pl.when(lat == side)
        def _():
            for xi in BONDS:
                if xi[1] * (1 - 2 * side) < 0:
                    put_weight(xi, True, range(xi[0], CX))

    for beta, c in PAIRS:
        if beta > 0:
            own_terms(0, beta, c, lambda x, q: 0 <= q < CX, force)
    for x in range(3, CX):
        advance(own[x], force[x])
    made = outer(right_tiles, lambda group, a: group.plane + a < CX)
    received("left_v", "over_left_v")
    advance_all(made)
    made = []
    for entry in right_rows:
        made += outer([entry], lambda group, a: a < 0)
    received("over_v")
    advance_all(made)
    third = blank()
    outer([(Row(0, 3), (1,), third)], lambda group, a: a >= 0)
    again = [blank() for _ in range(CX)]

    def early(x, q):
        return x >= 3 and q >= 3

    for beta, c in PAIRS:
        if beta <= 0:
            own_terms(1, beta, c, early, again)

    all_sent()
    received("right", "over_right")
    for plane in range(1, 6):
        spin(plane, OWN)
        turn(plane, OWN)
        spin(plane, halo)
        turn(plane, halo)
    for xi in BONDS:
        put_weight(xi, True, range(min(xi[0], CX)))
    for beta, c in PAIRS:
        own_terms(0, beta, c, lambda x, q: q < 0, force)
    for x in range(3):
        advance(own[x], force[x])
    made = outer([(Tile(-3), (0,)), (Tile(-2), every), (Tile(-1), every)])
    received("right_v", "over_right_v")
    advance_all(made)
    made = outer([(Row(-2, 1), every)]) + outer([(Row(-2, 2), every)])
    made += outer([(Row(0, 3), (1,), third)], lambda group, a: a < 0)
    advance_all(made)

    for beta, c in PAIRS:
        own_terms(1, beta, c, (lambda x, q: not early(x, q)) if beta <= 0 else (lambda x, q: True), again)
    for x in range(CX):
        for comp in range(3):
            speed = retain["own"] * (speeds[comp, x] + again[x][comp])
            half_out[comp, x] = F32(time_step) * speed
            base_out[comp, x] = frame[1, comp, X0 + x, OWN, :]


def local_steps(bars, displace, velocity, bond_low, bond_high, bc_type):
    any_space = pl.BlockSpec(memory_space=pl.ANY)
    out = pltpu.VMEM(displace.shape, F32)
    base, half = pl.pallas_call(
        functools.partial(kernel, bars),
        out_shape=(out, out),
        in_specs=[any_space] * 5,
        scratch_shapes=[
            pltpu.VMEM((STEPS, 3, PLANES, ROWS, NZ), F32),
            pltpu.VMEM((2, PLANES, ROWS, NZ), jnp.int32),
            pltpu.VMEM((3, PLANES, ROWS, NZ), F32),
            pltpu.VMEM((3, CX, RY, NZ), F32),
            pltpu.SMEM((bc_type.shape[0],), jnp.int32),
            pltpu.VMEM((5, 3, ROWS * LINE, NZ), F32),
            pltpu.VMEM((2, 5, ROWS * LINE, NZ), jnp.int32),
            pltpu.VMEM((STEPS, 5, 3, PLANES, ROWS, NZ), F32),
            pltpu.VMEM((2, 5, PLANES, ROWS, NZ), jnp.int32),
            pltpu.VMEM((7, 29, CX, RY, NZ), F32),
            pltpu.SemaphoreType.DMA((5,)),
            pltpu.SemaphoreType.DMA((len(SEND_GROUPS),)),
            pltpu.SemaphoreType.DMA((len(RECV_GROUPS),)),
        ],
        compiler_params=pltpu.CompilerParams(collective_id=0, has_side_effects=True),
        name="peridynamics",
    )(displace, velocity, bond_low, bond_high, bc_type)
    return base + half, half + half


def solution(mesh):
    bars = mesh.shape["bar"]
    return jax.shard_map(
        functools.partial(local_steps, bars),
        mesh=mesh,
        in_specs=(
            P(None, "bar", "lat", None),
            P(None, "bar", "lat", None),
            P("bar", "lat", None),
            P("bar", "lat", None),
            P(),
        ),
        out_specs=(P(None, "bar", "lat", None), P(None, "bar", "lat", None)),
        check_vma=False,
    )
```

```python
import functools

import jax
import jax.numpy as jnp
from jax import lax
from jax.experimental import pallas as pl
from jax.experimental.pallas import tpu as pltpu
from jax.sharding import PartitionSpec as P

STEPS = 2
modulus = 0.1
time_step = 0.5
MESH = pl.DeviceIdType.MESH

CX, RY, NZ = 6, 8, 128
PLANES, ROWS = 3 * CX + 5, 3 * RY
X0, Y0 = CX, RY
LINE = 25
OWN = slice(Y0, Y0 + RY)
F32 = jnp.float32


def bond_offsets():
    found = []
    for a in range(-3, 4):
        for b in range(-3, 4):
            for c in range(-3, 4):
                square = a * a + b * b + c * c
                if square == 0 or square > 9:
                    continue
                if a > 0 or (a == 0 and b > 0) or (a == 0 and b == 0 and c > 0):
                    found.append((a, b, c))
    return found


BONDS = bond_offsets()
NUMBER = {xi: k for k, xi in enumerate(BONDS)}
TURNS = (-2, -1, 1, 2)


def flag_of(xi):
    k = NUMBER[xi]
    return (0, 1 << k) if k < 31 else (1, 1 << (k - 31))


def bits_where(test):
    words = [0, 0]
    for xi in BONDS:
        if test(*xi):
            word, bit = flag_of(xi)
            words[word] |= bit
    return words


def disc(b):
    return [(a, c) for c in range(-3, 4) for a in range(-3, 4) if a * a + b * b + c * c <= 9]


PLACE = {abs(b): {ac: n for n, ac in enumerate(disc(b))} for b in range(4)}
PAIRS = [
    pair
    for c in range(0, 4)
    for b in range(-3, 4)
    if b * b + c * c <= 9 and (c > 0 or b >= 0)
    for pair in dict.fromkeys(((b, c), (-b, -c)))
]


def reach(b, c):
    return max(a for a in range(4) if a * a + b * b + c * c <= 9)


def strength(a, b, c):
    return time_step * (modulus / float(a * a + b * b + c * c) ** 1.5)


def combine(terms):
    terms = sorted(terms, key=lambda kv: isinstance(kv[0], (int, float)) and kv[0] < 0)
    out = None
    for k, v in terms:
        if not isinstance(k, (int, float)):
            out = v * k if out is None else out + v * k
            continue
        if k == 0:
            continue
        w = v if abs(k) == 1 else v * F32(abs(k))
        if out is None:
            out = w if k > 0 else -w
        else:
            out = out + w if k > 0 else out - w
    return out


SEND_GROUPS = (
    ("over", "over_v"),
    ("right", "over_right", "right_v", "over_right_v"),
    ("left", "over_left", "left_v", "over_left_v"),
)
RECV_GROUPS = (
    ("over",),
    ("left", "over_left"),
    ("right", "over_right"),
    ("over_v",),
    ("left_v", "over_left_v"),
    ("right_v", "over_right_v"),
)
SEND_SLOT = {name: slot for slot, names in enumerate(SEND_GROUPS) for name in names}
RECV_SLOT = {name: slot for slot, names in enumerate(RECV_GROUPS) for name in names}


def copies(side, refs, sems, bar, lat):
    u, v, flags = refs
    send, recv = sems

    def rows(ref, lead, src, dst, n):
        here = pl.ds(2 * RY - n - side * (RY - n), n)
        there = pl.ds(RY - n + side * (RY + n), n)
        return ref.at[lead, src, here], ref.at[lead, dst, there]

    def row(ref, lead, src, dst, n):
        here = pl.ds(2 * RY - n - side * (RY + 1 - 2 * n), 1)
        there = pl.ds(RY - n + side * (RY - 1 + 2 * n), 1)
        return ref.at[lead, src, here], ref.at[lead, dst, there]

    def tile(ref, lead, src, dst):
        return ref.at[lead, src, OWN], ref.at[lead, dst, OWN]

    every = slice(None)
    own = slice(6, 12)
    plan = {
        "over_right": [
            rows(u, every, slice(8, 12), slice(2, 6), 4),
            rows(flags, every, slice(8, 12), slice(2, 6), 4),
            row(u, every, slice(10, 12), slice(4, 6), 5),
            row(flags, every, slice(10, 12), slice(4, 6), 5),
            rows(u, every, slice(7, 8), slice(1, 2), 2),
            rows(flags, every, slice(7, 8), slice(1, 2), 2),
        ],
        "right": [
            tile(u, every, slice(7, 12), slice(1, 6)),
            tile(flags, 1, own, slice(0, 6)),
            tile(flags, 0, slice(8, 12), slice(2, 6)),
            tile(u, 0, slice(6, 7), slice(0, 1)),
        ],
        "over_left": [
            rows(u, every, slice(6, 11), slice(12, 17), 5),
            rows(flags, every, slice(6, 9), slice(12, 15), 5),
        ],
        "left": [
            tile(u, every, slice(6, 11), slice(12, 17)),
            tile(flags, every, slice(6, 9), slice(12, 15)),
            tile(u, 0, slice(11, 12), slice(17, 18)),
        ],
        "over": [rows(u, every, own, own, 5), rows(flags, every, own, own, 6), row(u, 1, own, own, 6)],
        "over_right_v": [rows(v, every, slice(10, 12), slice(4, 6), 2)],
        "right_v": [tile(v, every, slice(10, 12), slice(4, 6)), tile(v, 0, slice(9, 10), slice(3, 4))],
        "over_left_v": [rows(v, every, slice(6, 8), slice(12, 14), 2)],
        "left_v": [tile(v, every, slice(6, 8), slice(12, 14)), tile(v, 0, slice(8, 9), slice(14, 15))],
        "over_v": [rows(v, every, own, own, 2), row(v, 1, own, own, 3)],
    }
    partner = {
        "right": (bar + 1, lat),
        "left": (bar - 1, lat),
        "over": (bar, 1 - lat),
        "over_right": (bar + 1, 1 - lat),
        "over_left": (bar - 1, 1 - lat),
    }
    made = {}
    for name, pairs in plan.items():
        made[name] = []
        where = partner[name.removesuffix("_v")]
        for src, dst in pairs:
            made[name].append(
                functools.partial(
                    pltpu.make_async_remote_copy,
                    src_ref=src,
                    dst_ref=dst,
                    send_sem=send.at[SEND_SLOT[name]],
                    recv_sem=recv.at[RECV_SLOT[name]],
                    device_id={"bar": where[0], "lat": where[1]},
                    device_id_type=MESH,
                )
            )
    return made


def kernel(
    bars,
    u_hbm, v_hbm, low_hbm, high_hbm, bc_hbm,
    base_out, half_out,
    frame, flags, vel, speeds, bc, lines, marks, turned, spun, weight, local, send, recv,
):
    bar, lat = lax.axis_index("bar"), lax.axis_index("lat")
    has_left, has_right = bar > 0, bar < bars - 1
    flat_frame = frame.reshape(STEPS, 3, PLANES * ROWS, NZ)
    flat_vel = vel.reshape(3, PLANES * ROWS, NZ)
    flat_turned = turned.reshape(STEPS, 5, 3, PLANES * ROWS, NZ)

    loads = [
        pltpu.make_async_copy(low_hbm, flags.at[0, X0:X0 + CX, OWN], local.at[0]),
        pltpu.make_async_copy(high_hbm, flags.at[1, X0:X0 + CX, OWN], local.at[1]),
        pltpu.make_async_copy(u_hbm, frame.at[0, :, X0:X0 + CX, OWN], local.at[2]),
        pltpu.make_async_copy(v_hbm, vel.at[:, X0:X0 + CX, OWN], local.at[3]),
        pltpu.make_async_copy(bc_hbm, bc, local.at[4]),
    ]
    barrier = pltpu.get_barrier_semaphore()

    def greet(b, l):
        pl.semaphore_signal(barrier, inc=1, device_id={"bar": b, "lat": l}, device_id_type=MESH)

    @pl.when(has_right)
    def _():
        greet(bar + 1, 1 - lat)
        greet(bar + 1, lat)

    @pl.when(has_left)
    def _():
        greet(bar - 1, 1 - lat)
        greet(bar - 1, lat)

    greet(bar, 1 - lat)

    for copy in loads:
        copy.start()

    void = pl.ds(pl.multiple_of(lat * (2 * RY), RY), RY)
    halo_start = pl.multiple_of((1 - lat) * (2 * RY), RY)
    halo = pl.ds(halo_start, RY)
    for step, first, last in ((0, 1, 17), (1, 4, 14)):
        zero = jnp.zeros((last - first, RY, NZ), F32)
        for comp in range(3):
            if comp < 2:
                frame[step, comp, first:last, void, :] = zero
            for c in TURNS:
                turned[step, c + 2, comp, first:last, void, :] = zero
    for word in range(2):
        flags[word, 0:15, void, :] = jnp.full((15, RY, NZ), -1, jnp.int32)
        for c in TURNS:
            spun[word, c + 2, 1:15, void, :] = jnp.full((14, RY, NZ), -1, jnp.int32)

    @pl.when(jnp.logical_not(has_left))
    def _():
        for comp in range(3):
            frame[0, comp, 0:6] = jnp.zeros((6, ROWS, NZ), F32)
            vel[comp, 3:6] = jnp.zeros((3, ROWS, NZ), F32)
        for word in range(2):
            flags[word, 0:6] = jnp.full((6, ROWS, NZ), -1, jnp.int32)

    @pl.when(jnp.logical_not(has_right))
    def _():
        for comp in range(3):
            frame[0, comp, 12:18] = jnp.zeros((6, ROWS, NZ), F32)
            vel[comp, 12:15] = jnp.zeros((3, ROWS, NZ), F32)

    sems = (send, recv)
    refs = (frame.at[0], vel, flags)
    sent = copies(lat, refs, sems, bar, lat)

    def when_there(condition, run):
        if condition is None:
            run()
        else:
            pl.when(condition)(run)

    def send_all():
        even = lax.rem(bar, 2) == 0
        odd = jnp.logical_not(even)
        order = (
            ('over', even),
            ('over_v', even),
            ('over_right', None),
            ('right', None),
            ('right_v', None),
            ('over_right_v', None),
            ('over', odd),
            ('over_left', None),
            ('left', None),
            ('over_v', odd),
            ('over_left_v', None),
            ('left_v', None),
        )
        for name, there in order:
            made = sent[name]
            if there is None:
                there = {"right": has_right, "left": has_left}.get(name.removesuffix("_v").split("_")[-1])

            def run():
                for copy in made:
                    copy().start()

            when_there(there, run)

    def wait_group(names, sem, there):
        lines_sent = sum(
            copy.keywords["src_ref"].shape[0] * copy.keywords["src_ref"].shape[1] * copy.keywords["src_ref"].shape[2]
            if len(copy.keywords["src_ref"].shape) == 4
            else copy.keywords["src_ref"].shape[0] * copy.keywords["src_ref"].shape[1]
            for name in names
            for copy in sent[name]
        )

        def run():
            total = lines.at[0, 0, 0:lines_sent]
            pltpu.make_async_copy(total, total, sem).wait()

        when_there(there, run)

    def received(*names):
        there = {"right": has_left, "left": has_right}.get(names[0].removesuffix("_v"))
        wait_group(names, recv.at[RECV_GROUPS.index(names)], there)

    def all_sent():
        for slot, there in enumerate((None, has_right, has_left)):
            wait_group(SEND_GROUPS[slot], send.at[slot], there)

    row = lax.broadcasted_iota(jnp.int32, (RY, NZ), 0)
    lane = lax.broadcasted_iota(jnp.int32, (RY, NZ), 1)
    for copy in loads[:2]:
        copy.wait()
    for word in range(2):
        gone = jnp.zeros((RY, NZ), jnp.int32)
        for t in range(3):
            under = bits_where(lambda a, b, c: b < -t)[word]
            above = bits_where(lambda a, b, c: b > t)[word]
            cut = jnp.where(lat == 0, jnp.int32(under), jnp.int32(above))
            gone = jnp.where(row == t + lat * (RY - 1 - 2 * t), cut, gone)
        for t in range(3):
            under = bits_where(lambda a, b, c: c < -t)[word]
            above = bits_where(lambda a, b, c: c > t)[word]
            gone = jnp.where(lane == t, gone | jnp.int32(under), gone)
            gone = jnp.where(lane == NZ - 1 - t, gone | jnp.int32(above), gone)
        for x in range(CX):
            flags[word, X0 + x, OWN, :] = flags[word, X0 + x, OWN, :] | gone

    @pl.when(jnp.logical_not(has_right))
    def _():
        for x in range(3, CX):
            beyond = bits_where(lambda a, b, c: x + a >= CX)
            for word in range(2):
                flags[word, X0 + x, OWN, :] = flags[word, X0 + x, OWN, :] | jnp.int32(beyond[word])

    for copy in loads[2:]:
        copy.wait()
    sign = 1 - 2 * lat
    fsign = sign.astype(F32)
    edge_row = {d: Y0 + RY - 1 + d - lat * (RY - 1 + 2 * d) for d in (1, 2, 3)}

    class Tile:
        def __init__(self, plane):
            self.plane = plane

        def get(self, ref, lead, a, b):
            return ref[(*lead, X0 + self.plane + a, pl.ds(Y0 + b, RY), slice(None))]

        def put(self, ref, flat, lead, value):
            ref[(*lead, X0 + self.plane, OWN, slice(None))] = value

    class Row:
        def __init__(self, plane, d):
            self.plane, self.d = plane, d

        def get(self, ref, lead, a, b):
            at = pl.ds(edge_row[self.d] * LINE + ((X0 + self.plane + a) + b * LINE), RY)
            if ref is frame:
                return lines[2, lead[1], at, :]
            if ref is turned:
                return lines[lead[1], lead[2], at, :]
            if ref is flags:
                return marks[lead[0], 2, at, :]
            if ref is spun:
                return marks[lead[0], lead[1], at, :]
            return flat_vel[(*lead, self.strided(), slice(None))]

        def strided(self):
            return pl.ds(edge_row[self.d] + (X0 + self.plane) * ROWS, RY, stride=ROWS)

        def put(self, ref, flat, lead, value):
            flat[(*lead, self.strided(), slice(None))] = value

    def line(plane, rows):
        return pl.ds((Y0 * LINE if rows is OWN else halo_start * LINE) + plane, RY, stride=LINE)

    def spin(plane, rows, turns=(-2, -1, 0, 1, 2)):
        for word in range(2):
            held = flags[word, plane, rows, :]
            for c in turns:
                moved = pltpu.roll(held, (-c) % NZ, axis=1) if c else held
                marks[word, c + 2, line(plane, rows), :] = moved
                if c:
                    spun[word, c + 2, plane, rows, :] = moved

    def turn(plane, rows, turns=(-2, -1, 0, 1, 2)):
        for comp in range(3):
            held = frame[0, comp, plane, rows, :]
            for c in turns:
                moved = combine([(c if comp == 2 else 1, pltpu.roll(held, (-c) % NZ, axis=1))]) if c else held
                lines[c + 2, comp, line(plane, rows), :] = moved
                if c:
                    turned[0, c + 2, comp, plane, rows, :] = moved

    def put_weight(xi, back, planes):
        a, b, c = xi
        word, bit = flag_of(xi)
        a1, b1, c1 = (-a, -b, -c) if back else xi
        place = PLACE[abs(b1)][(a1, c1)]
        for x in planes:
            if not back:
                held = flags[word, X0 + x, OWN, :]
            elif c == 0:
                held = flags[word, X0 + x + a1, Y0 + b1:Y0 + b1 + RY, :]
            elif c == 3:
                held = pltpu.roll(flags[word, X0 + x, OWN, :], 3, axis=1)
            else:
                held = spun[word, c1 + 2, X0 + x + a1, Y0 + b1:Y0 + b1 + RY, :]
            weight[b1 + 3, place, x] = jnp.where((held & jnp.int32(bit)) == 0, F32(strength(*xi)), F32(0.0))

    heres = {}

    def add_terms(step, b, shift, factor, c, tasks):
        seen = {}
        opposite = (step, -b, -c)
        for key in list(heres):
            if key[:3] != opposite:
                del heres[key]
        for group, todo, force, want, table in tasks:
            if 0 not in want:
                todo = todo if (b or c) and (1 not in want or b or 2 in want) else []
            elif want == (0,):
                todo = [a for a in todo if a]
            todo = [a for a in todo if a or b or c]
            if not todo:
                continue

            def fetch(comp, a):
                if c == 0:
                    return group.get(frame, (step, comp), a, shift)
                return group.get(turned, (step, c + 2, comp), a, shift)

            def mine(comp):
                return group.get(frame, (step, comp), 0, 0)

            def nearby(a):
                key = (group.plane + a, isinstance(group, Row) and group.d)
                if key not in seen:
                    terms = []
                    if abs(c) == 3:
                        terms.append((c, pltpu.roll(mine(2), (-c) % NZ, axis=1)))
                    elif c:
                        terms.append((1, fetch(2, a)))
                    if b:
                        terms.append((factor, fetch(1, a)))
                    seen[key] = combine(terms)
                return seen[key]

            def kept(a, value):
                if table is not None:
                    return table[PLACE[abs(b)][(a, c)], group.plane] * value
                if (a, b, c) in NUMBER:
                    word, bit = flag_of((a, b, c))
                    held = group.get(flags, (word,), 0, 0)
                else:
                    word, bit = flag_of((-a, -b, -c))
                    if c == 0:
                        held = group.get(flags, (word,), a, b)
                    elif c == -3:
                        held = pltpu.roll(group.get(flags, (word,), 0, 0), 3, axis=1)
                    else:
                        held = group.get(spun, (word, c + 2), a, b)
                return jnp.where((held & jnp.int32(bit)) == 0, value, F32(0.0))

            needs = [a for a in todo if (*opposite, -a, group) not in heres]
            mine0 = mine(0) if any(needs) else None
            alone = not b and not c
            base = combine([(factor, mine(1))] * bool(b) + [(c, mine(2))] * bool(c)) if needs else None
            pulls = {}
            for a in todo:
                if alone:
                    pulls[a] = kept(a, fetch(0, a) - mine0)
                    continue
                there = nearby(a)
                if a:
                    there = combine([(1, there), (a, fetch(0, a))])
                if a in needs:
                    here = combine([(1, base), (a, mine0)]) if a else base
                    heres[(step, b, c, a, group)] = here
                    pulls[a] = kept(a, there - here)
                else:
                    pulls[a] = kept(a, there + heres[(*opposite, -a, group)])
            total, along = None, None
            for size in range(4):
                plus, minus = pulls.get(size), pulls.get(-size) if size else None
                if plus is None and minus is None:
                    continue
                k = 1.0 if table is not None else strength(size, b, c)
                if alone:
                    both = combine([(1, v) for v in (plus, minus) if v is not None])
                    along = combine([(1, along)] * (along is not None) + [(k * size * size, both)])
                    continue
                both = combine([(1, v) for v in (plus, minus) if v is not None])
                total = combine([(1, total)] * (total is not None) + [(k, both)])
                if size and 0 in want:
                    if plus is None:
                        term = (-k * size, minus)
                    elif minus is None:
                        term = (k * size, plus)
                    else:
                        term = (k * size, plus - minus)
                    along = combine([(1, along)] * (along is not None) + [term])
            for comp, k, value in ((0, 1, along), (1, factor, total), (2, c, total)):
                if comp not in want or value is None or (comp == 1 and not b) or (comp == 2 and not c):
                    continue
                force[comp] = combine([(1, force[comp])] * (force[comp] is not None) + [(k, value)])

    retain = {}
    for key, where in (("left", jnp.maximum(bar - 1, 0)), ("own", bar), ("right", jnp.minimum(bar + 1, bars - 1))):
        retain[key] = 1.0 - 0.2 * bc[where].astype(F32)

    def retain_of(group):
        if isinstance(group, Tile):
            return retain["left" if group.plane < 0 else "own" if group.plane < CX else "right"]
        plane = row + group.plane
        return jnp.where(plane < 0, retain["left"], jnp.where(plane < CX, retain["own"], retain["right"]))

    def advance(group, force, want=(0, 1, 2)):
        keep = retain_of(group)
        for comp in want:
            speed = keep * (group.get(vel, (comp,), 0, 0) + force[comp])
            moved = group.get(frame, (0, comp), 0, 0) + F32(time_step) * speed
            if isinstance(group, Tile) and 0 <= group.plane < CX:
                speeds[comp, group.plane] = speed
            group.put(frame, flat_frame, (1, comp), moved)
            far = (group.plane in (-3, 8)) if isinstance(group, Tile) else group.d == 3
            if not far:
                for c in TURNS:
                    value = pltpu.roll(moved, (-c) % NZ, axis=1)
                    group.put(turned, flat_turned, (1, c + 2, comp), combine([(c if comp == 2 else 1, value)]))

    def blank():
        return [None, None, None]

    def span(b, c):
        far = reach(b, c)
        return range(-far, far + 1)

    own = [Tile(x) for x in range(CX)]
    force = [blank() for _ in range(CX)]
    every = (0, 1, 2)

    def own_terms(step, beta, c, chosen, pulls):
        shift, factor = (sign * beta, fsign * F32(beta)) if beta else (0, 0)
        table = weight.at[3 + shift]
        tasks = [
            (own[x], [a for a in span(beta, c) if chosen(x, x + a)], pulls[x], every, table) for x in range(CX)
        ]
        add_terms(step, beta, shift, factor, c, tasks)

    def outer(groups_wants, chosen=lambda group, a: True):
        made = [(entry[0], entry[2] if len(entry) > 2 else blank(), entry[1]) for entry in groups_wants]
        for b, c in PAIRS:
            add_terms(
                0, b, b, b, c,
                [(group, [a for a in span(b, c) if chosen(group, a)], pull, want, None) for group, pull, want in made],
            )
        return made

    def advance_all(made):
        for group, pull, want in made:
            advance(group, pull, want)

    pl.semaphore_wait(barrier, 1 + 2 * has_left.astype(jnp.int32) + 2 * has_right.astype(jnp.int32))
    send_all()

    for x in range(CX):
        spin(X0 + x, OWN)
        turn(X0 + x, OWN)
    for xi in BONDS:
        put_weight(xi, False, range(CX))
    for xi in BONDS:
        if xi[1] == 0:
            put_weight(xi, True, range(xi[0], CX))
    for side in range(2):

        @pl.when(lat == side)
        def _():
            for xi in BONDS:
                if xi[1] * (1 - 2 * side) > 0:
                    put_weight(xi, True, range(xi[0], CX))

    for beta, c in PAIRS:
        if beta <= 0:
            own_terms(0, beta, c, lambda x, q: 0 <= q < CX, force)

    received("left", "over_left")
    for plane in range(12, 17):
        turn(plane, OWN)
        turn(plane, halo)
    for plane in range(12, 15):
        spin(plane, OWN)
        spin(plane, halo)
    for b, c in PAIRS:
        add_terms(0, b, b, b, c, [
            (own[x], [a for a in span(b, c) if x + a >= CX], force[x], every, weight.at[3 + b]) for x in range(CX)
        ])
    right_tiles = [(Tile(6), every, blank()), (Tile(7), every, blank()), (Tile(8), (0,), blank())]
    right_rows = [(Row(6, d), every, blank()) for d in (1, 2)]
    outer(right_tiles, lambda group, a: group.plane + a >= CX)
    for entry in right_rows:
        outer([entry], lambda group, a: a >= 0)

    received("over")
    for x in range(CX):
        spin(X0 + x, halo)
        turn(X0 + x, halo)
    for side in range(2):

        @pl.when(lat == side)
        def _():
            for xi in BONDS:
                if xi[1] * (1 - 2 * side) < 0:
                    put_weight(xi, True, range(xi[0], CX))

    for beta, c in PAIRS:
        if beta > 0:
            own_terms(0, beta, c, lambda x, q: 0 <= q < CX, force)
    for x in range(3, CX):
        advance(own[x], force[x])
    made = outer(right_tiles, lambda group, a: group.plane + a < CX)
    received("left_v", "over_left_v")
    advance_all(made)
    made = []
    for entry in right_rows:
        made += outer([entry], lambda group, a: a < 0)
    received("over_v")
    advance_all(made)
    third = blank()
    outer([(Row(0, 3), (1,), third)], lambda group, a: a >= 0)
    again = [blank() for _ in range(CX)]

    def early(x, q):
        return x >= 3 and q >= 3

    for beta, c in PAIRS:
        if beta <= 0:
            own_terms(1, beta, c, early, again)

    all_sent()
    received("right", "over_right")
    for plane in range(1, 6):
        spin(plane, OWN)
        turn(plane, OWN)
        spin(plane, halo)
        turn(plane, halo)
    for xi in BONDS:
        put_weight(xi, True, range(min(xi[0], CX)))
    for beta, c in PAIRS:
        own_terms(0, beta, c, lambda x, q: q < 0, force)
    for x in range(3):
        advance(own[x], force[x])
    made = outer([(Tile(-3), (0,)), (Tile(-2), every), (Tile(-1), every)])
    received("right_v", "over_right_v")
    advance_all(made)
    made = outer([(Row(-2, 1), every)]) + outer([(Row(-2, 2), every)])
    made += outer([(Row(0, 3), (1,), third)], lambda group, a: a < 0)
    advance_all(made)

    for beta, c in PAIRS:
        own_terms(1, beta, c, (lambda x, q: not early(x, q)) if beta <= 0 else (lambda x, q: True), again)
    for x in range(CX):
        for comp in range(3):
            speed = retain["own"] * (speeds[comp, x] + again[x][comp])
            half_out[comp, x] = F32(time_step) * speed
            base_out[comp, x] = frame[1, comp, X0 + x, OWN, :]


def local_steps(bars, displace, velocity, bond_low, bond_high, bc_type):
    any_space = pl.BlockSpec(memory_space=pl.ANY)
    out = pltpu.VMEM(displace.shape, F32)
    base, half = pl.pallas_call(
        functools.partial(kernel, bars),
        out_shape=(out, out),
        in_specs=[any_space] * 5,
        scratch_shapes=[
            pltpu.VMEM((STEPS, 3, PLANES, ROWS, NZ), F32),
            pltpu.VMEM((2, PLANES, ROWS, NZ), jnp.int32),
            pltpu.VMEM((3, PLANES, ROWS, NZ), F32),
            pltpu.VMEM((3, CX, RY, NZ), F32),
            pltpu.SMEM((bc_type.shape[0],), jnp.int32),
            pltpu.VMEM((5, 3, ROWS * LINE, NZ), F32),
            pltpu.VMEM((2, 5, ROWS * LINE, NZ), jnp.int32),
            pltpu.VMEM((STEPS, 5, 3, PLANES, ROWS, NZ), F32),
            pltpu.VMEM((2, 5, PLANES, ROWS, NZ), jnp.int32),
            pltpu.VMEM((7, 29, CX, RY, NZ), F32),
            pltpu.SemaphoreType.DMA((5,)),
            pltpu.SemaphoreType.DMA((len(SEND_GROUPS),)),
            pltpu.SemaphoreType.DMA((len(RECV_GROUPS),)),
        ],
        compiler_params=pltpu.CompilerParams(collective_id=0, has_side_effects=True),
        name="peridynamics",
    )(displace, velocity, bond_low, bond_high, bc_type)
    return base + half, half + half


def solution(mesh):
    bars = mesh.shape["bar"]
    return jax.shard_map(
        functools.partial(local_steps, bars),
        mesh=mesh,
        in_specs=(
            P(None, "bar", "lat", None),
            P(None, "bar", "lat", None),
            P("bar", "lat", None),
            P("bar", "lat", None),
            P(),
        ),
        out_specs=(P(None, "bar", "lat", None), P(None, "bar", "lat", None)),
        check_vma=False,
    )
```
